256 devices in a mesh: gx: 8 (over z_lo, core), gy: 4 (over x), gz: 8 (over y, z_hi).
Axes of the slice: x: 4, y: 4, z: 8 (z_hi: 2, z_lo: 4; z = z_hi * 4 + z_lo), core: 2. Of those that a mesh axis runs over, the one named last changes fastest.
Arguments:
- displacement: float32 [3, 48, 24, 3072], P(None, 'gx', 'gy', 'gz'), may hold values from -0.18 to 0.18
- size_field_modes: float32 [27, 16, 8, 1024], P(None, 'gx', 'gy', 'gz'), may hold values from -6 to 6
- velocity: float32 [3, 16, 8, 1024], P(None, 'gx', 'gy', 'gz'), may hold values from -1 to 1
Outputs:
- advected_field: float32 [27, 16, 8, 1024], P(None, 'gx', 'gy', 'gz')
- gradient: float32 [3, 48, 24, 3072], P(None, 'gx', 'gy', 'gz')
- checks: float32 [3], replicated
The draws below stay inside these ranges and needn't reach their ends.
All inputs are finite; a program needn't handle non-finite values. Where the reference program divides by a largest or mean magnitude, that divisor is 1e-20 or more.
Results may differ from the reference program's by a relative error of at most 0.0001.
Values sent between devices are 32-bit elements; how exact they have to be, the bound alone decides.
A program may use at most 64 MiB of HBM per device.

```python
import math
import jax
import jax.numpy as jnp
import numpy as np
from jax import lax

LOCAL_ELEMS_X = 2
LOCAL_ELEMS_Y = 2
LOCAL_ELEMS_Z = 128
SUBSTEPS = 4
GLOBAL_ELEMS_X = 16
GLOBAL_ELEMS_Y = 8
GLOBAL_ELEMS_Z = 1024
ELEMENTS = 131072


def draw_size_field_modes(key, part):
    random_key_noise, random_key_blocks = jax.random.split(key)
    noise_component = jnp.clip(0.5 * jax.random.normal(random_key_noise, (27, GLOBAL_ELEMS_X, GLOBAL_ELEMS_Y, GLOBAL_ELEMS_Z), jnp.float32), -3.0, 3.0)
    block_list = jax.random.uniform(random_key_blocks, (GLOBAL_ELEMS_X // LOCAL_ELEMS_X, GLOBAL_ELEMS_Y // LOCAL_ELEMS_Y, GLOBAL_ELEMS_Z // LOCAL_ELEMS_Z), jnp.float32, -3.0, 3.0)
    offset = jnp.repeat(jnp.repeat(jnp.repeat(block_list, LOCAL_ELEMS_X, axis=0), LOCAL_ELEMS_Y, axis=1), LOCAL_ELEMS_Z, axis=2)
    return noise_component.at[0].add(offset)


def draw_velocity(key, part):
    random_key_heading, random_key_scale = jax.random.split(key)
    heading_text = jax.random.uniform(random_key_heading, (3, GLOBAL_ELEMS_X, GLOBAL_ELEMS_Y, GLOBAL_ELEMS_Z), jnp.float32, -1.0, 1.0)
    scale_factors = jnp.exp(jax.random.uniform(random_key_scale, (GLOBAL_ELEMS_X // LOCAL_ELEMS_X, GLOBAL_ELEMS_Y // LOCAL_ELEMS_Y, GLOBAL_ELEMS_Z // LOCAL_ELEMS_Z), jnp.float32, math.log(0.15), 0.0))
    expanded = jnp.repeat(jnp.repeat(jnp.repeat(scale_factors, LOCAL_ELEMS_X, axis=0), LOCAL_ELEMS_Y, axis=1), LOCAL_ELEMS_Z, axis=2)
    return heading_text * expanded[None]


def block_levels(rng, shape, shards, low, largest):
    gain = 1.0
    for axis_at, blocks in shards:
        draws = jax.random.uniform(jax.random.fold_in(jax.random.fold_in(rng, 6), axis_at), (blocks,), jnp.float32, low / len(shards), largest / len(shards))
        gain = gain * jnp.repeat(jnp.exp(draws), shape[axis_at] // blocks).reshape((-1,) + (1,) * (len(shape) - 1 - axis_at))
    return gain


def normal_values(own_key, shape, scale, most, cuts=(), kind=jnp.bfloat16):
    drawn = jax.random.normal(own_key, shape, jnp.float32) * scale
    if len(cuts) > 0:
        drawn = block_levels(own_key, shape, cuts, -0.22, 0.18) * drawn
    return jnp.clip(drawn, min=-most, max=most).astype(kind)


def setup_inputs(seed: int = 0) -> dict:
    key_list = jax.random.split(jax.random.key(seed), 4)
    displacement = normal_values(key_list[0], (3, 3 * GLOBAL_ELEMS_X, 3 * GLOBAL_ELEMS_Y, 3 * GLOBAL_ELEMS_Z), 0.03, 0.18, ((1, 8), (2, 4), (3, 8)), jnp.float32)
    size_field_modes = draw_size_field_modes(jax.random.fold_in(key_list[3], 71), 0)
    velocity = draw_velocity(jax.random.fold_in(key_list[3], 71), 0)
    return {"displacement": displacement, "size_field_modes": size_field_modes, "velocity": velocity}


root_half = 0.7071067811865476
root_three_half = 1.224744871391589
root_five_half = 1.5811388300841898
plus_values = (0.7071067811865476, 1.224744871391589, 1.5811388300841898)
minus_values = (0.7071067811865476, -1.224744871391589, 1.5811388300841898)
stiffness = ((0.0, 0.0, 0.0), (1.7320508075688772, 0.0, 0.0), (0.0, 3.872983346207417, 0.0))
courant = 0.1
theta_size = 0.3
trial_step = 0.05

def build_tables():
    points = np.array([-0.8611363115940526, -0.3399810435848563, 0.3399810435848563, 0.8611363115940526])
    weights = np.array([0.3478548451374538, 0.6521451548625461, 0.6521451548625461, 0.3478548451374538])
    points = 0.5 * (points + 1.0)
    weights = 0.5 * weights
    node_points = np.array([0.0, 1.0 / 3.0, 2.0 / 3.0, 1.0])
    value_table = np.zeros((4, 4))
    slope_table = np.zeros((4, 4))
    for column in range(4):
        others = [node_points[member] for member in range(4) if member != column]
        denominator = np.prod([node_points[column] - member for member in others])
        for quad_row in range(4):
            gauss_point = points[quad_row]
            value_table[quad_row, column] = np.prod([gauss_point - member for member in others]) / denominator
            slope_table[quad_row, column] = sum((np.prod([gauss_point - others[position] for position in range(3) if position != skipped]) for skipped in range(3))) / denominator
    centred = 2.0 * points - 1.0
    legendre_table = np.stack([np.full(4, root_half), root_three_half * centred, root_five_half * 0.5 * (3.0 * centred ** 2 - 1.0)], axis=1)
    cube_table = (weights[:, None, None] * weights[None, :, None] * weights[None, None, :]).reshape(4, 4, 4, 1, 1, 1)
    return (value_table, slope_table, legendre_table, cube_table)

def as_table(operand):
    return jnp.asarray(np.asarray(operand), jnp.float32)

def contract(weights_table, operand, along):
    product = jnp.tensordot(as_table(weights_table), operand, axes=([1], [along]), precision=lax.Precision.HIGHEST)
    return jnp.moveaxis(product, 0, along)

def trace_along(modal_coefficients, vector, direction):
    return jnp.tensordot(as_table(vector), modal_coefficients, axes=([0], [direction]), precision=lax.Precision.HIGHEST)

def spread_shape(vector, direction):
    broadcast_shape = [1] * 6
    broadcast_shape[direction] = 3
    return as_table(vector).reshape(broadcast_shape)

def boundary_terms(modal_coefficients, local_speed, right_ext, left_ext, speed_ext, direction):
    extent = modal_coefficients.shape[3 + direction]
    face_speed = 0.5 * (lax.slice_in_dim(speed_ext, 0, extent + 1, axis=direction) + lax.slice_in_dim(speed_ext, 1, extent + 2, axis=direction))
    flux = jnp.maximum(face_speed, 0.0)[None, None] * right_ext + jnp.minimum(face_speed, 0.0)[None, None] * left_ext
    flux_left = lax.slice_in_dim(flux, 0, extent, axis=2 + direction)
    flux_right = lax.slice_in_dim(flux, 1, extent + 1, axis=2 + direction)
    lifted = contract(stiffness, modal_coefficients, direction)
    faces = spread_shape(plus_values, direction) * jnp.expand_dims(flux_right, direction) - spread_shape(minus_values, direction) * jnp.expand_dims(flux_left, direction)
    return local_speed[None, None, None] * lifted - faces

def element_energy(corners, modal_coefficients):
    lagrange_values, lagrange_slopes, legendre_values, cube_weights = build_tables()
    along_value = contract(lagrange_values, corners, 1)
    along_slope = contract(lagrange_slopes, corners, 1)
    value_value = contract(lagrange_values, along_value, 2)
    jac_first = contract(lagrange_values, contract(lagrange_values, along_slope, 2), 3)
    jac_second = contract(lagrange_values, contract(lagrange_slopes, along_value, 2), 3)
    jac_third = contract(lagrange_slopes, value_value, 3)
    columns = (jac_first, jac_second, jac_third)
    sample = contract(legendre_values, contract(legendre_values, contract(legendre_values, modal_coefficients, 0), 1), 2)
    target_size = jnp.exp(theta_size * sample)
    inverse = 1.0 / target_size
    mapped = [[((1.0 if component == column else 0.0) + columns[column][component]) * inverse for column in range(3)] for component in range(3)]
    metric = jnp.zeros_like(sample)
    for first_column in range(3):
        for second_column in range(3):
            gram_entry = mapped[0][first_column] * mapped[0][second_column] + mapped[1][first_column] * mapped[1][second_column] + mapped[2][first_column] * mapped[2][second_column]
            deviation = gram_entry - (1.0 if first_column == second_column else 0.0)
            metric = metric + deviation * deviation
    return jnp.sum(as_table(cube_weights) * target_size ** 3 * metric)

def element_corners(padded):
    gathered = padded
    for along, stack_axis in ((1, 1), (3, 2), (5, 3)):
        extent = (gathered.shape[along] - 1) // 3
        gathered = jnp.stack([lax.slice_in_dim(gathered, node_offset, node_offset + 3 * extent - 2, stride=3, axis=along) for node_offset in range(4)], axis=stack_axis)
    return gathered

def pad_one(operand, node_offset, along):
    config = [(0, 0, 0)] * operand.ndim
    config[along] = (node_offset, 3 - node_offset, 2)
    return lax.pad(operand, jnp.zeros((), operand.dtype), config)

def spread_corners(corner_grad):
    spread = corner_grad
    for stack_axis, along in ((3, 5), (2, 3), (1, 1)):
        pieces = [pad_one(lax.index_in_dim(spread, node_offset, axis=stack_axis, keepdims=False), node_offset, along) for node_offset in range(4)]
        spread = pieces[0] + pieces[1] + pieces[2] + pieces[3]
    return spread

def advection_rate(modal_coefficients, velocity):
    accumulated = jnp.zeros_like(modal_coefficients)
    for direction in range(3):
        element_axis = 2 + direction
        extent = modal_coefficients.shape[3 + direction]
        local_speed = velocity[direction]
        speed_ext = jnp.concatenate([lax.slice_in_dim(local_speed, extent - 1, extent, axis=direction), local_speed, lax.slice_in_dim(local_speed, 0, 1, axis=direction)], axis=direction)
        right_trace = trace_along(modal_coefficients, plus_values, direction)
        left_trace = trace_along(modal_coefficients, minus_values, direction)
        right_ext = jnp.concatenate([lax.slice_in_dim(right_trace, extent - 1, extent, axis=element_axis), right_trace], axis=element_axis)
        left_ext = jnp.concatenate([left_trace, lax.slice_in_dim(left_trace, 0, 1, axis=element_axis)], axis=element_axis)
        accumulated = accumulated + boundary_terms(modal_coefficients, local_speed, right_ext, left_ext, speed_ext, direction)
    return 2.0 * accumulated

def periodic_pad(nodal):
    for along in (1, 2, 3):
        nodal = jnp.concatenate([nodal, lax.slice_in_dim(nodal, 0, 1, axis=along)], axis=along)
    return nodal

def periodic_fold(gradient_pad):
    for along in (1, 2, 3):
        extent = gradient_pad.shape[along] - 1
        gradient_pad = jnp.concatenate([lax.slice_in_dim(gradient_pad, 0, 1, axis=along) + lax.slice_in_dim(gradient_pad, extent, extent + 1, axis=along), lax.slice_in_dim(gradient_pad, 1, extent, axis=along)], axis=along)
    return gradient_pad

def gradient_scan(padded, modal_coefficients):

    def advance(running, slab_start):
        energy_sum, gradient_pad = running
        nodes_slab = lax.dynamic_slice_in_dim(padded, 3 * slab_start, 4, axis=1)
        field_slab = lax.dynamic_slice_in_dim(modal_coefficients, slab_start, 1, axis=3)
        energy_here, corner_grad = jax.value_and_grad(element_energy)(element_corners(nodes_slab), field_slab)
        contribution = spread_corners(corner_grad)
        current = lax.dynamic_slice_in_dim(gradient_pad, 3 * slab_start, 4, axis=1)
        gradient_pad = lax.dynamic_update_slice_in_dim(gradient_pad, current + contribution, 3 * slab_start, axis=1)
        return ((energy_sum + energy_here, gradient_pad), None)
    start_value = (jnp.zeros((), jnp.float32), jnp.zeros_like(padded))
    finished, unused = lax.scan(advance, start_value, jnp.arange(GLOBAL_ELEMS_X, dtype=jnp.int32))
    return finished

def energy_scan(padded, modal_coefficients):

    def advance(energy_sum, slab_start):
        nodes_slab = lax.dynamic_slice_in_dim(padded, 3 * slab_start, 4, axis=1)
        field_slab = lax.dynamic_slice_in_dim(modal_coefficients, slab_start, 1, axis=3)
        return (energy_sum + element_energy(element_corners(nodes_slab), field_slab), None)
    finished, unused = lax.scan(advance, jnp.zeros((), jnp.float32), jnp.arange(GLOBAL_ELEMS_X, dtype=jnp.int32))
    return finished

def reference(displacement, size_field_modes, velocity):
    modal_coefficients = size_field_modes.reshape(3, 3, 3, GLOBAL_ELEMS_X, GLOBAL_ELEMS_Y, GLOBAL_ELEMS_Z)
    fastest = jnp.max(lax.optimization_barrier(jnp.sum(jnp.abs(velocity), axis=0)))
    time_step = courant / jnp.maximum(fastest, 0.25)
    for substep in range(SUBSTEPS):
        midway = modal_coefficients + time_step * advection_rate(modal_coefficients, velocity)
        modal_coefficients = 0.5 * modal_coefficients + 0.5 * (midway + time_step * advection_rate(midway, velocity))
    energy_total, gradient_pad = gradient_scan(periodic_pad(displacement), modal_coefficients)
    gradient = periodic_fold(gradient_pad)
    elements = 1.0 * ELEMENTS
    entries = 81.0 * ELEMENTS
    square_total = jnp.sum(gradient * gradient)
    step_length = trial_step / jnp.sqrt(1.0 + square_total / entries)
    trial_nodes = displacement - step_length * gradient
    trial_total = energy_scan(periodic_pad(trial_nodes), modal_coefficients)
    checks = jnp.stack([energy_total / elements, square_total / entries, trial_total / elements])
    return (modal_coefficients.reshape(27, GLOBAL_ELEMS_X, GLOBAL_ELEMS_Y, GLOBAL_ELEMS_Z), gradient, checks)
```

```python
import functools

import jax
import jax.numpy as jnp
import numpy as np
from jax import lax
from jax.experimental import pallas as pl
from jax.experimental.pallas import tpu as pltpu
from jax.sharding import PartitionSpec as P

MESH = pl.DeviceIdType.MESH
ROUNDS = 4
C0, C1, C2 = 0.7071067811865476, 1.224744871391589, 1.5811388300841898
ROOT3, ROOT15 = 1.7320508075688772, 3.872983346207417
FACE = C0 * C0 + C1 * C1 + C2 * C2
COURANT = 0.1
THETA = 0.3
TRIAL = 0.05
F32 = jnp.float32
BF16 = jnp.bfloat16


def tables():
    points = np.array(
        [-0.8611363115940526, -0.3399810435848563, 0.3399810435848563, 0.8611363115940526]
    )
    weights = 0.5 * np.array(
        [0.3478548451374538, 0.6521451548625461, 0.6521451548625461, 0.3478548451374538]
    )
    centred = points
    points = 0.5 * (points + 1.0)
    nodes = np.array([0.0, 1.0 / 3.0, 2.0 / 3.0, 1.0])
    value = np.zeros((4, 4))
    slope = np.zeros((4, 4))
    for column in range(4):
        others = [nodes[m] for m in range(4) if m != column]
        below = np.prod([nodes[column] - m for m in others])
        for row in range(4):
            t = points[row]
            value[row, column] = np.prod([t - m for m in others]) / below
            slope[row, column] = (
                sum(np.prod([t - others[i] for i in range(3) if i != k]) for k in range(3)) / below
            )
    legendre = np.stack(
        [np.full(4, C0), C1 * centred, C2 * 0.5 * (3.0 * centred**2 - 1.0)], axis=1
    )
    cube = np.einsum("p,q,r->pqr", weights, weights, weights).reshape(64)
    wide = np.zeros((2, 2, 3, 4, 4, 4, 4, 7, 8))
    for x in range(2):
        for y in range(2):
            for d in range(3):
                t = [slope if d == axis else value for axis in range(3)]
                wide[x, y, d, :, :, :, :, 3 * x : 3 * x + 4, 3 * y : 3 * y + 4] = np.einsum(
                    "pi,qj,rk->pqrkij", t[0], t[1], t[2]
                )
    wide = wide.reshape(768, 224)
    return legendre, cube, wide


def halves(a):
    hi = np.asarray(a, np.float32).astype(jnp.bfloat16)
    lo = (np.asarray(a, np.float64) - hi.astype(np.float64)).astype(jnp.bfloat16)
    return hi, lo


def split(x):
    hi = x.astype(BF16)
    return hi, (x - hi.astype(F32)).astype(BF16)


def dot(a, b):
    return lax.dot_general(a, b, (((1,), (0,)), ((), ())), preferred_element_type=F32)


def roll(x, by, axis):
    by %= x.shape[axis]
    return x if by == 0 else pltpu.roll(x, by, axis)


def take(ref, d, i):
    return ref[i] if d == 0 else (ref[:, i] if d == 1 else ref[:, :, i])


def kernel(
    nx,
    ny,
    nz,
    disp_ref,
    modes_ref,
    vel_ref,
    wf_any,
    wb_any,
    perm_any,
    cube_ref,
    adv_ref,
    grad_ref,
    checks_ref,
    wf_ref,
    wb_ref,
    perm_ref,
    term,
    vel,
    zs_out,
    zs_in,
    face_out,
    face_in,
    diag_out,
    diag_in,
    tx_out,
    tx_in,
    ty_out,
    ty_in,
    td_out,
    td_in,
    din,
    t0,
    t1,
    nf,
    jac,
    s_ref,
    om_ref,
    q_ref,
    gh,
    gl,
    pg,
    gx_out,
    gx_in,
    gy_out,
    gy_in,
    gd_out,
    gd_in,
    nt,
    hh,
    max_a,
    max_b,
    sum_a,
    sum_b,
    acc_ref,
    local_sem,
    z_sem,
    face_sem,
    diag_sem,
    t_sem,
    g_sem,
    red_sem,
):
    gx, gy, gz = lax.axis_index("gx"), lax.axis_index("gy"), lax.axis_index("gz")

    def at(dx, dy, dz=0):
        return (
            lax.rem(gx + (dx + nx), nx) if dx else gx,
            lax.rem(gy + (dy + ny), ny) if dy else gy,
            lax.rem(gz + (dz + nz), nz) if dz else gz,
        )

    half = nz // 2
    group_a = [
        (i * half + j, (gx, lax.rem(gy + i, ny), lax.rem(gz + 2 * j, nz)))
        for i in range(ny)
        for j in range(half)
        if (i, j) != (0, 0)
    ]
    flipped = gz + 1 - 2 * lax.rem(gz, 2)
    group_b = [
        (i * 2 + b, (lax.rem(gx + i, nx), gy, flipped if b else gz))
        for i in range(nx)
        for b in range(2)
        if (i, b) != (0, 0)
    ]
    count_a, count_b = ny * half, 2 * nx
    corners = ((1, 1), (1, -1), (-1, 1), (-1, -1))
    sides = ((1, 0), (-1, 0), (0, 1), (0, -1))
    partners = [at(*s) for s in sides + corners] + [at(0, 0, 1), at(0, 0, -1)]
    partners += [p for _, p in group_a] + [p for _, p in group_b]

    barrier = pltpu.get_barrier_semaphore()
    for p in partners:
        pl.semaphore_signal(barrier, inc=1, device_id=p, device_id_type=MESH)

    loads = [
        pltpu.make_async_copy(a, b, local_sem.at[i])
        for i, (a, b) in enumerate(((perm_any, perm_ref), (wf_any, wf_ref), (wb_any, wb_ref)))
    ]
    for c in loads:
        c.start()

    pending = []

    def remote(src, dst, send, recv, to):
        c = pltpu.make_async_remote_copy(
            src_ref=src, dst_ref=dst, send_sem=send, recv_sem=recv, device_id=to, device_id_type=MESH
        )
        c.start()
        pending.append(c)
        return c

    row = lax.broadcasted_iota(jnp.int32, (8, 128), 0)
    lane = lax.broadcasted_iota(jnp.int32, (8, 128), 1)
    xlow = ((row // 2) % 2) == 0
    ylow = (row % 2) == 0
    top = row < 4

    term[0] = jnp.zeros((3, 3, 3, 8, 128), F32)
    vel[...] = jnp.zeros((3, 8, 128), F32)
    for a in range(3):
        for b in range(3):
            for c in range(3):
                term[0, a, b, c, 0:4, :] = modes_ref[a * 9 + b * 3 + c]
        vel[a, 0:4, :] = vel_ref[a]
    speed = jnp.abs(vel[0]) + jnp.abs(vel[1]) + jnp.abs(vel[2])
    fastest = jnp.max(jnp.max(speed, axis=1, keepdims=True), axis=0, keepdims=True)
    max_a[0] = jnp.broadcast_to(fastest, (1, 128))

    def packed_of(i):
        lo = term[0, (2 * i) // 9, (2 * i) // 3 % 3, (2 * i) % 3] if 2 * i < 27 else vel[2 * i - 27]
        j = 2 * i + 1
        hi = term[0, j // 9, j // 3 % 3, j % 3] if j < 27 else vel[j - 27]
        return jnp.where(top, lo, roll(hi, 4, 0))

    for v in range(2):
        low = jnp.zeros((8, 128), F32)
        high = jnp.zeros((8, 128), F32)
        for i in range(8 * v, min(8 * v + 8, 15)):
            q = i % 8
            w = packed_of(i)
            mine = (lane >= 16 * q) & (lane < 16 * q + 16)
            low = jnp.where(mine, roll(w, 16 * q, 1), low)
            high = jnp.where(mine, roll(w, 16 * q + 16, 1), high)
        zs_out[0, v] = low
        zs_out[1, v] = high

    din[...] = jnp.zeros((144, 384), F32)
    for c in range(3):
        for x in range(6):
            din[(c * 6 + x) * 8 : (c * 6 + x) * 8 + 6, :] = disp_ref[c, x]
    whole = din[...]
    hi = whole.astype(BF16)
    rest = whole - hi.astype(F32)
    mid = rest.astype(BF16)
    lo = (rest - mid.astype(F32)).astype(BF16)
    loads[0].wait()
    perm = perm_ref[...]
    din[...] = dot(hi, perm) + (dot(mid, perm) + dot(lo, perm))
    t0[...] = jnp.zeros((504, 128), F32)
    low = jnp.zeros((8, 128), F32)
    high = jnp.zeros((8, 128), F32)
    for k in range(3):
        for c in range(3):
            for x in range(6):
                t = k * 3 + c
                j = t * 6 + x
                piece = din[(c * 6 + x) * 8 : (c * 6 + x) * 8 + 8, k * 128 : k * 128 + 128]
                t0[t * 56 + x * 8 : t * 56 + x * 8 + 8, :] = piece
                mine = (lane >= 2 * j) & (lane < 2 * j + 2)
                low = jnp.where(mine, roll(piece, 2 * j, 1), low)
                high = jnp.where(mine, roll(piece, 2 * j + 2, 1), high)
    zs_out[0, 2] = low
    zs_out[1, 2] = high

    pl.semaphore_wait(barrier, len(partners))

    z_up = remote(zs_out.at[1], zs_in.at[1], z_sem.at[0], z_sem.at[1], at(0, 0, 1))
    z_down = remote(zs_out.at[0], zs_in.at[0], z_sem.at[2], z_sem.at[3], at(0, 0, -1))
    maxes_a = [
        remote(max_a.at[0], max_a.at[s], red_sem.at[0, 0, s], red_sem.at[0, 1, s], p)
        for s, p in group_a
    ]
    z_up.wait_recv()
    z_down.wait_recv()
    for v in range(2):
        from_low = zs_in[1, v]
        from_high = zs_in[0, v]
        for i in range(8 * v, min(8 * v + 8, 15)):
            q = i % 8
            near = jnp.where(
                lane < 16,
                roll(from_high, 128 - 16 * q, 1),
                jnp.where(lane >= 112, roll(from_low, 112 - 16 * q, 1), 0.0),
            )
            for j, part in ((2 * i, roll(near, 4, 0)), (2 * i + 1, near)):
                if j < 27:
                    old = term[0, j // 9, j // 3 % 3, j % 3]
                    term[0, j // 9, j // 3 % 3, j % 3] = jnp.where(top, old, part)
                else:
                    vel[j - 27] = jnp.where(top, vel[j - 27], part)

    def zprev(x):
        axis = x.ndim - 1
        r = roll(x, 1, axis)
        return jnp.where(lane == 0, roll(r, 4, axis - 1), r)

    def znext(x):
        axis = x.ndim - 1
        r = roll(x, 127, axis)
        return jnp.where(lane == 127, roll(r, 4, axis - 1), r)

    v0, v1, v2 = vel[0], vel[1], vel[2]
    zero = jnp.zeros((8, 128), F32)
    inner = (
        jnp.where(xlow, 0.0, COURANT * (v0 + roll(v0, 2, 0))),
        jnp.where(ylow, 0.0, COURANT * (v1 + roll(v1, 1, 0))),
        COURANT * (v2 + zprev(v2)),
    )
    plus = [jnp.maximum(f, 0.0) for f in inner]
    minus = [jnp.minimum(f, 0.0) for f in inner]
    grow1 = [(2.0 * COURANT * ROOT3) * v for v in (v0, v1, v2)]
    grow2 = [(2.0 * COURANT * ROOT15) * v for v in (v0, v1, v2)]
    lows = (xlow, ylow)
    signs = (jnp.where(xlow, 1.0, -1.0), jnp.where(ylow, 1.0, -1.0))

    def outward(parts, d):
        e = C0 * parts[0] + C2 * parts[2]
        o = C1 * parts[1]
        return jnp.where(lows[d], e - o, e + o)

    def local_rate(src, dst):
        rims = []
        for d in range(3):
            u0, u1, u2 = take(src, d, 0), take(src, d, 1), take(src, d, 2)
            e = C0 * u0 + C2 * u2
            o = C1 * u1
            tp = e + o
            tm = e - o
            if d < 2:
                rims.append(jnp.where(lows[d], tm, tp))
                by = 2 - d
                lower = plus[d] * roll(tp, by, 2) + minus[d] * tm
                upper = roll(lower, 8 - by, 2)
            else:
                lower = plus[d] * zprev(tp) + minus[d] * tm
                upper = znext(lower)
            drop = lower - upper
            outs = (
                C0 * drop,
                grow1[d] * u0 - C1 * (lower + upper),
                grow2[d] * u1 + C2 * drop,
            )
            for i in range(3):
                if d == 0:
                    dst[i] = outs[i]
                elif d == 1:
                    dst[:, i] = dst[:, i] + outs[i]
                else:
                    dst[:, :, i] = dst[:, :, i] + outs[i]
        return rims

    def add_face(dst, d, flux):
        signed = signs[d] * flux
        outs = (C0 * signed, -C1 * flux, C2 * signed)
        for i in range(3):
            if d == 0:
                dst[i] = dst[i] + outs[i]
            else:
                dst[:, i] = dst[:, i] + outs[i]

    def sides_of(f, d):
        p, m = jnp.maximum(f, 0.0), jnp.minimum(f, 0.0)
        return jnp.where(lows[d], p, m), jnp.where(lows[d], m, p)

    def meet(a, b, d):
        by = 2 - d
        return jnp.where(lows[d], roll(a, 8 - by, a.ndim - 2), roll(b, by, b.ndim - 2))

    def corner_of(r):
        e = [roll(diag_in[r, i], by, 1) for i, by in enumerate((5, 7, 1, 3))]
        return jnp.where(xlow, jnp.where(ylow, e[0], e[1]), jnp.where(ylow, e[2], e[3]))

    speeds = {}

    def advance(r, hidden):
        src, mid_ref, dst = term.at[2 * r], term.at[2 * r + 1], term.at[2 * r + 2]
        rims = local_rate(src, mid_ref)
        n = 11 if r == 0 else 9
        m = 5 if r == 0 else 3
        for d in range(2):
            by = 2 - d
            far = outward([take(mid_ref, d, i) for i in range(3)], d)
            up = jnp.where(lows[d], roll(far, 8 - by, 2), rims[d])
            down = jnp.where(lows[d], rims[d], roll(far, by, 2))
            for i in range(3):
                face_out[r, 2 * d, 3 * i : 3 * i + 3] = up[i]
                face_out[r, 2 * d + 1, 3 * i : 3 * i + 3] = down[i]
            if r == 0:
                for w in range(2):
                    face_out[r, 2 * d + w, 9] = v0
                    face_out[r, 2 * d + w, 10] = v1
        diag_out[r, 0:3] = outward([rims[0][0], rims[0][1], rims[0][2]], 1)
        if r == 0:
            diag_out[r, 3] = v0
            diag_out[r, 4] = v1
        copies = [
            remote(
                diag_out.at[r, pl.ds(0, m)],
                diag_in.at[r, i, pl.ds(0, m)],
                diag_sem.at[r, 0, i],
                diag_sem.at[r, 1, i],
                at(*s),
            )
            for i, s in enumerate(corners)
        ]
        copies += [
            remote(
                face_out.at[r, i, pl.ds(0, n)],
                face_in.at[r, i, pl.ds(0, n)],
                face_sem.at[r, 0, i],
                face_sem.at[r, 1, i],
                at(*s),
            )
            for i, s in enumerate(sides)
        ]
        hidden()
        for c in copies:
            c.wait_recv()
        if r == 0:
            corner = corner_of(0)
            cv0, cv1 = corner[3], corner[4]
            beside = [meet(face_in[0, 2 * d, 9:11], face_in[0, 2 * d + 1, 9:11], d) for d in (0, 1)]
            speeds["rim"] = (
                sides_of(COURANT * (v0 + beside[0][0]), 0),
                sides_of(COURANT * (v1 + beside[1][1]), 1),
            )
            speeds["far"] = (
                sides_of(COURANT * (beside[0][1] + cv1), 1),
                sides_of(COURANT * (beside[1][0] + cv0), 0),
            )
            edge = corner[0:3]
        else:
            edge = corner_of(r)[0:3]
        ghosts = []
        for d in range(2):
            a = face_in[r, 2 * d, 0:9].reshape(3, 3, 8, 128)
            b = face_in[r, 2 * d + 1, 0:9].reshape(3, 3, 8, 128)
            ghost = meet(a, b, d)
            partial = jnp.where(lows[d], a, b)
            theirs, own = speeds["rim"][d]
            flux = theirs * ghost + own * rims[d]
            add_face(mid_ref, d, flux)
            other = 1 - d
            beyond, inside = speeds["far"][d]
            side_flux = beyond * edge + inside * outward([ghost[0], ghost[1], ghost[2]], other)
            signed = signs[other] * side_flux
            whole_face = partial - (FACE * signs[d]) * flux
            ghosts.append(
                (
                    whole_face[0] + C0 * signed,
                    whole_face[1] - C1 * side_flux,
                    whole_face[2] + C2 * signed,
                )
            )
        rims = local_rate(mid_ref, dst)
        for d in range(2):
            theirs, own = speeds["rim"][d]
            flux = [theirs * ghosts[d][i] + own * rims[d][i] for i in range(3)]
            for j in range(3):
                signed = signs[d] * flux[j]
                for i, value in enumerate((C0 * signed, -C1 * flux[j], C2 * signed)):
                    if d == 0:
                        dst[i, j] = dst[i, j] + value
                    else:
                        dst[j, i] = dst[j, i] + value

    later = {}

    def hidden0():
        tx_out[9] = zs_in[0, 2]
        tx_out[10] = zs_in[1, 2]
        for t in range(9):
            tx_out[t] = t0[t * 56 : t * 56 + 8, :]
        ty_out[...] = jnp.zeros((80, 128), F32)
        ty_out[0:63, :] = t0[pl.ds(0, 63, stride=8), :]
        td_out[...] = jnp.zeros((32, 128), F32)
        td_out[0:9, :] = t0[pl.ds(0, 9, stride=56), :]
        for out, base in ((ty_out, 64), (td_out, 16)):
            out[base : base + 8, :] = zs_in[0, 2]
            out[base + 8 : base + 16, :] = zs_in[1, 2]
        later["t"] = [
            remote(tx_out, tx_in, t_sem.at[0, 0], t_sem.at[1, 0], at(-1, 0)),
            remote(ty_out, ty_in, t_sem.at[0, 1], t_sem.at[1, 1], at(0, -1)),
            remote(td_out, td_in, t_sem.at[0, 2], t_sem.at[1, 2], at(-1, -1)),
        ]
        for c in maxes_a:
            c.wait_recv()
        best = max_a[0]
        for s in range(1, count_a):
            best = jnp.maximum(best, max_a[s])
        max_b[0] = best
        later["max"] = [
            remote(max_b.at[0], max_b.at[s], red_sem.at[1, 0, s], red_sem.at[1, 1, s], p)
            for s, p in group_b
        ]

    def hidden1():
        for c in later["t"]:
            c.wait_recv()
        for t in range(9):
            t0[t * 56 + 48 : t * 56 + 56, :] = tx_in[t]
        t0[pl.ds(6, 63, stride=8), :] = ty_in[0:63, :]
        t0[pl.ds(54, 9, stride=56), :] = td_in[0:9, :]
        packs = []
        for w in range(2):
            own = jnp.where(
                row < 6, zs_in[w, 2], jnp.where(row == 6, roll(ty_in[64 + 8 * w : 72 + 8 * w, :], 6, 0), 0.0)
            )
            rim = jnp.where(
                row < 6, tx_in[9 + w], jnp.where(row == 6, roll(td_in[16 + 8 * w : 24 + 8 * w, :], 6, 0), 0.0)
            )
            packs.append((own, rim))
        for t in range(9):
            for x in range(7):
                j = t * 6 + x % 6
                from_high, from_low = packs[0][x // 6], packs[1][x // 6]
                t1[t * 56 + x * 8 : t * 56 + x * 8 + 8, :] = jnp.where(
                    lane < 2,
                    roll(from_high, 128 - 2 * j, 1),
                    jnp.where(lane >= 126, roll(from_low, 126 - 2 * j, 1), 0.0),
                )
        wide_lane = lax.broadcasted_iota(jnp.int32, (56, 128), 1)
        for c in range(3):
            for k in range(3):
                t = k * 3 + c
                nf[k * 56 : k * 56 + 56, c * 256 : c * 256 + 128] = t0[t * 56 : t * 56 + 56, :]
                nf[k * 56 : k * 56 + 56, c * 256 + 128 : c * 256 + 256] = t1[t * 56 : t * 56 + 56, :]
            a = roll(t0[c * 56 : c * 56 + 56, :], 127, 1)
            b = roll(t1[c * 56 : c * 56 + 56, :], 127, 1)
            nf[168:224, c * 256 : c * 256 + 128] = jnp.where(wide_lane == 127, b, a)
            nf[168:224, c * 256 + 128 : c * 256 + 256] = jnp.where(wide_lane == 127, a, b)

    def hidden2():
        loads[1].wait()
        for c in range(3):
            a, b = split(nf[:, c * 256 : c * 256 + 256])
            jac[:, c * 256 : c * 256 + 256] = (
                dot(wf_ref[0:768, :], a) + dot(wf_ref[768:1536, :], a) + dot(wf_ref[0:768, :], b)
            )

    series = np.polynomial.polynomial.polypow([1.0, 1.0, 0.5], 4)

    def hidden3():
        for c in later["max"]:
            c.wait_recv()
        best = max_b[0]
        for s in range(1, count_b):
            best = jnp.maximum(best, max_b[s])
        tau = jnp.broadcast_to(1.0 / jnp.maximum(best, 0.25), (8, 128))
        acc = float(series[6]) * term[6]
        for k in range(5, -1, -1):
            acc = acc * tau + float(series[k]) * term[k]
        acc_ref[...] = acc
        tau2 = tau * tau
        tau4 = tau2 * tau2
        later["tau"] = (tau4 * tau2 * tau, tau4 * tau4)
        loads[2].wait()

    for r, hidden in enumerate((hidden0, hidden1, hidden2, hidden3)):
        advance(r, hidden)

    legendre, _, _ = tables()
    tau7, tau8 = later["tau"]
    field = acc_ref[...] + ((float(series[7]) * tau7) * term[7] + (float(series[8]) * tau8) * term[8])
    acc_ref[...] = field
    for a in range(3):
        for b in range(3):
            for c in range(3):
                adv_ref[a * 9 + b * 3 + c] = field[a, b, c, 0:4]
    lg = [[float(v) for v in line] for line in legendre]
    for p in range(4):
        along = lg[p][0] * acc_ref[0] + lg[p][1] * acc_ref[1] + lg[p][2] * acc_ref[2]
        for q in range(4):
            second = lg[q][0] * along[0] + lg[q][1] * along[1] + lg[q][2] * along[2]
            for r in range(4):
                g = p * 16 + q * 4 + r
                s_ref[g * 8 : g * 8 + 8, :] = (
                    lg[r][0] * second[0] + lg[r][1] * second[1] + lg[r][2] * second[2]
                )

    pairs = ((0, 0, 1.0), (1, 1, 1.0), (2, 2, 1.0), (0, 1, 2.0), (0, 2, 2.0), (1, 2, 2.0))

    def jacobian(col, g, tile):
        return [
            [
                jac[pl.ds(pl.multiple_of(col * 192 + d * 64 + g * 16, 16), 16), c * 256 + tile * 128 : c * 256 + tile * 128 + 128]
                + (1.0 if c == d else 0.0)
                for d in range(3)
            ]
            for c in range(3)
        ]

    def strain(jm, q):
        a = {}
        for d, e, _ in pairs:
            k = q * (jm[0][d] * jm[0][e] + jm[1][d] * jm[1][e] + jm[2][d] * jm[2][e])
            a[d, e] = a[e, d] = k - 1.0 if d == e else k
        return a

    def inner_product(a, b):
        on = a[0, 0] * b[0, 0] + a[1, 1] * b[1, 1] + a[2, 2] * b[2, 2]
        off = a[0, 1] * b[0, 1] + a[0, 2] * b[0, 2] + a[1, 2] * b[1, 2]
        return on + 2.0 * off

    def forces(step, energy):
        col, g = step // 4, step % 4
        w = cube_ref[pl.ds(pl.multiple_of(g * 16, 16), 16), :]
        for tile in range(2):
            s = s_ref[pl.ds(g * 128 + tile * 4 + col, 16, stride=8), :]
            size = jnp.exp(THETA * s)
            q = jnp.exp((-2.0 * THETA) * s)
            jm = jacobian(col, g, tile)
            a = strain(jm, q)
            if tile == 0:
                om = w * (size * size * size)
                energy = energy + om * inner_product(a, a)
                at_row = pl.ds(pl.multiple_of(col * 64 + g * 16, 16), 16)
                om_ref[at_row, :] = om
                q_ref[at_row, :] = q
            fac = (4.0 * w) * size
            for d in range(3):
                rows = pl.ds(pl.multiple_of(col * 192 + d * 64 + g * 16, 16), 16)
                for c in range(3):
                    value = fac * (jm[c][0] * a[0, d] + jm[c][1] * a[1, d] + jm[c][2] * a[2, d])
                    hi, lo = split(value)
                    gh[rows, c * 256 + tile * 128 : c * 256 + tile * 128 + 128] = hi
                    gl[rows, c * 256 + tile * 128 : c * 256 + tile * 128 + 128] = lo
        return energy

    energy = lax.fori_loop(0, 16, forces, jnp.zeros((16, 128), F32))

    wide_lane = lax.broadcasted_iota(jnp.int32, (56, 128), 1)
    rim = jnp.zeros((56, 128), F32)
    for c in range(3):
        a = gh[:, c * 256 : c * 256 + 256]
        b = gl[:, c * 256 : c * 256 + 256]
        part = dot(wb_ref[0:224, :], a) + dot(wb_ref[224:448, :], a) + dot(wb_ref[0:224, :], b)
        r0 = roll(part[168:224, 0:128], 1, 1)
        r1 = roll(part[168:224, 128:256], 1, 1)
        pg[c * 56 : c * 56 + 56, :] = part[0:56, 0:128] + jnp.where(wide_lane == 0, r1, r0)
        for k in (1, 2):
            pg[(k * 3 + c) * 56 : (k * 3 + c) * 56 + 56, :] = part[k * 56 : k * 56 + 56, 0:128]
        last = part[0:56, 128:256] + r0
        rim = jnp.where(wide_lane == c, roll(last, c, 1), rim)
    pg[504:560, :] = rim

    for t in range(10):
        gx_out[0, t] = pg[t * 56 + 48 : t * 56 + 56, :]
        gx_out[1, t] = pg[t * 56 : t * 56 + 8, :]
    for i, start in enumerate((54, 48, 6, 0)):
        gd_out[i] = jnp.zeros((16, 128), F32)
        gd_out[i, 0:10, :] = pg[pl.ds(start, 10, stride=56), :]
    for i, start in enumerate((6, 0)):
        gy_out[i] = jnp.zeros((72, 128), F32)
        gy_out[i, 0:70, :] = pg[pl.ds(start, 70, stride=8), :]
    moved = [
        remote(gd_out.at[i], gd_in.at[i], g_sem.at[0, 4 + i], g_sem.at[1, 4 + i], at(*s))
        for i, s in enumerate(corners)
    ]
    moved += [
        remote(gx_out.at[i], gx_in.at[i], g_sem.at[0, i], g_sem.at[1, i], at(*sides[i])) for i in range(2)
    ]
    moved += [
        remote(gy_out.at[i], gy_in.at[i], g_sem.at[0, 2 + i], g_sem.at[1, 2 + i], at(*sides[2 + i]))
        for i in range(2)
    ]
    def total(x):
        return jnp.sum(jnp.sum(x, axis=0, keepdims=True), axis=1, keepdims=True)

    energy = total(energy)
    for c in moved:
        c.wait_recv()
    for t in range(10):
        pg[t * 56 : t * 56 + 8, :] = pg[t * 56 : t * 56 + 8, :] + gx_in[0, t]
        pg[t * 56 + 48 : t * 56 + 56, :] = pg[t * 56 + 48 : t * 56 + 56, :] + gx_in[1, t]
    for i, start in enumerate((0, 6)):
        pg[pl.ds(start, 70, stride=8), :] = pg[pl.ds(start, 70, stride=8), :] + gy_in[i, 0:70, :]
    for i, start in enumerate((0, 6, 48, 54)):
        pg[pl.ds(start, 10, stride=56), :] = pg[pl.ds(start, 10, stride=56), :] + gd_in[i, 0:10, :]

    entries = 81.0 * 512.0 * nx * ny * nz
    own = jnp.zeros((8, 128), F32)
    outer = jnp.zeros((8, 128), F32)
    for t in range(10):
        for x in range(7):
            piece = pg[t * 56 + x * 8 : t * 56 + x * 8 + 8, :]
            if t < 9 and x < 6:
                own = own + piece * piece
            else:
                outer = outer + piece * piece
    square = total(jnp.where(row < 6, own, 0.0))
    reach = total(jnp.where(row < 6, outer, own + outer)) + square
    reach_step = TRIAL / jnp.sqrt(1.0 + reach / entries)

    for c in range(3):
        for k in range(3):
            t = k * 3 + c
            nt[k * 56 : k * 56 + 56, c * 128 : c * 128 + 128] = reach_step * pg[t * 56 : t * 56 + 56, :]
        nt[168:224, c * 128 : c * 128 + 128] = reach_step * jnp.where(
            wide_lane == 127, roll(pg[504:560, :], 127 - c, 1), roll(pg[c * 56 : c * 56 + 56, :], 127, 1)
        )
    a, b = split(nt[...])
    hh[...] = dot(wf_ref[0:768, :], a) + dot(wf_ref[768:1536, :], a) + dot(wf_ref[0:768, :], b)

    def coefficients(step, sums):
        col, g = step // 4, step % 4
        at_row = pl.ds(pl.multiple_of(col * 64 + g * 16, 16), 16)
        om, q = om_ref[at_row, :], q_ref[at_row, :]
        jm = jacobian(col, g, 0)
        hm = [
            [
                hh[pl.ds(pl.multiple_of(col * 192 + d * 64 + g * 16, 16), 16), c * 128 : c * 128 + 128]
                for d in range(3)
            ]
            for c in range(3)
        ]
        a = strain(jm, q)
        b, cc = {}, {}
        for d, e, _ in pairs:
            if d == e:
                k = (2.0 * q) * (jm[0][d] * hm[0][d] + jm[1][d] * hm[1][d] + jm[2][d] * hm[2][d])
            else:
                k = q * (
                    (jm[0][d] * hm[0][e] + jm[1][d] * hm[1][e] + jm[2][d] * hm[2][e])
                    + (jm[0][e] * hm[0][d] + jm[1][e] * hm[1][d] + jm[2][e] * hm[2][d])
                )
            b[d, e] = k
            cc[d, e] = q * (hm[0][d] * hm[0][e] + hm[1][d] * hm[1][e] + hm[2][d] * hm[2][e])
        return (
            sums[0] - om * (2.0 * inner_product(a, b)),
            sums[1] + om * (inner_product(b, b) + 2.0 * inner_product(a, cc)),
            sums[2] - om * (2.0 * inner_product(b, cc)),
            sums[3] + om * inner_product(cc, cc),
        )

    none = jnp.zeros((16, 128), F32)
    sums = lax.fori_loop(0, 16, coefficients, (none, none, none, none))
    line = lax.broadcasted_iota(jnp.int32, (1, 128), 1)
    values = [energy, square, reach_step] + [total(s) for s in sums]
    mine = jnp.zeros((1, 128), F32)
    for i, value in enumerate(values):
        mine = jnp.where(line == i, value, mine)
    sum_a[0] = mine
    sums_a = [
        remote(sum_a.at[0], sum_a.at[s], red_sem.at[2, 0, s], red_sem.at[2, 1, s], p)
        for s, p in group_a
    ]

    for c in range(3):
        for x in range(6):
            for k in range(3):
                t = k * 3 + c
                din[(c * 6 + x) * 8 : (c * 6 + x) * 8 + 8, k * 128 : k * 128 + 128] = pg[
                    t * 56 + x * 8 : t * 56 + x * 8 + 8, :
                ]
    whole = din[...]
    hi = whole.astype(BF16)
    rest = whole - hi.astype(F32)
    mid = rest.astype(BF16)
    lo = (rest - mid.astype(F32)).astype(BF16)
    perm = perm_ref[...]

    def back(x):
        return lax.dot_general(x, perm, (((1,), (1,)), ((), ())), preferred_element_type=F32)

    din[...] = back(hi) + (back(mid) + back(lo))
    for c in range(3):
        for x in range(6):
            grad_ref[c, x] = din[(c * 6 + x) * 8 : (c * 6 + x) * 8 + 6, :]

    def weigh(ratio):
        two = ratio * ratio
        return jnp.where(
            line == 3,
            ratio,
            jnp.where(line == 4, two, jnp.where(line == 5, two * ratio, jnp.where(line == 6, two * two, 1.0))),
        )

    def pick(v, i):
        return jnp.sum(jnp.where(line == i, v, 0.0), axis=1, keepdims=True)

    def combine(ref, count):
        steps = [pick(ref[s], 2) for s in range(count)]
        least = functools.reduce(jnp.minimum, steps)
        out = jnp.zeros((1, 128), F32)
        for s in range(count):
            out = out + ref[s] * weigh(least / steps[s])
        return jnp.where(line == 2, least, out)

    for c in sums_a:
        c.wait_recv()
    sum_b[0] = combine(sum_a, count_a)
    sums_b = [
        remote(sum_b.at[0], sum_b.at[s], red_sem.at[3, 0, s], red_sem.at[3, 1, s], p)
        for s, p in group_b
    ]
    for c in sums_b:
        c.wait_recv()
    final = combine(sum_b, count_b)
    square = pick(final, 1)
    step_length = TRIAL / jnp.sqrt(1.0 + square / entries)
    grown = final * weigh(step_length / pick(final, 2))
    elements = 512.0 * nx * ny * nz
    trial = jnp.sum(jnp.where((line == 0) | ((line >= 3) & (line < 7)), grown, 0.0))
    checks_ref[0] = jnp.sum(jnp.where(line == 0, final, 0.0)) * (1.0 / elements)
    checks_ref[1] = jnp.sum(jnp.where(line == 1, final, 0.0)) * (1.0 / entries)
    checks_ref[2] = trial * (1.0 / elements)

    for c in pending:
        c.wait_send()


def solution(mesh):
    nx, ny, nz = mesh.shape["gx"], mesh.shape["gy"], mesh.shape["gz"]
    _, cube, wide = tables()
    hi, lo = halves(wide)
    wf = np.concatenate([hi, lo], axis=0)
    wb = np.concatenate([hi.T, lo.T], axis=0)
    perm = np.zeros((384, 384), np.float32)
    for k in range(3):
        perm[3 * np.arange(128) + k, k * 128 + np.arange(128)] = 1.0
    perm = perm.astype(jnp.bfloat16)
    cube = np.broadcast_to(np.asarray(cube, np.float32)[:, None], (64, 128))
    count_a, count_b = ny * (nz // 2), 2 * nx
    most = max(count_a, count_b)
    vmem = pl.BlockSpec(memory_space=pltpu.VMEM)
    anywhere = pl.BlockSpec(memory_space=pl.ANY)
    dma = pltpu.SemaphoreType.DMA
    call = pl.pallas_call(
        functools.partial(kernel, nx, ny, nz),
        name="tmop_step",
        out_shape=(
            jax.ShapeDtypeStruct((27, 4, 128), F32),
            jax.ShapeDtypeStruct((3, 6, 6, 384), F32),
            jax.ShapeDtypeStruct((3,), F32),
        ),
        in_specs=[vmem, vmem, vmem, anywhere, anywhere, anywhere, vmem],
        out_specs=(vmem, vmem, pl.BlockSpec(memory_space=pltpu.SMEM)),
        scratch_shapes=[
            pltpu.VMEM((1536, 224), BF16),
            pltpu.VMEM((448, 768), BF16),
            pltpu.VMEM((384, 384), BF16),
            pltpu.VMEM((2 * ROUNDS + 1, 3, 3, 3, 8, 128), F32),
            pltpu.VMEM((3, 8, 128), F32),
            pltpu.VMEM((2, 3, 8, 128), F32),
            pltpu.VMEM((2, 3, 8, 128), F32),
            pltpu.VMEM((ROUNDS, 4, 11, 8, 128), F32),
            pltpu.VMEM((ROUNDS, 4, 11, 8, 128), F32),
            pltpu.VMEM((ROUNDS, 5, 8, 128), F32),
            pltpu.VMEM((ROUNDS, 4, 5, 8, 128), F32),
            pltpu.VMEM((11, 8, 128), F32),
            pltpu.VMEM((11, 8, 128), F32),
            pltpu.VMEM((80, 128), F32),
            pltpu.VMEM((80, 128), F32),
            pltpu.VMEM((32, 128), F32),
            pltpu.VMEM((32, 128), F32),
            pltpu.VMEM((144, 384), F32),
            pltpu.VMEM((504, 128), F32),
            pltpu.VMEM((504, 128), F32),
            pltpu.VMEM((224, 768), F32),
            pltpu.VMEM((768, 768), F32),
            pltpu.VMEM((512, 128), F32),
            pltpu.VMEM((256, 128), F32),
            pltpu.VMEM((256, 128), F32),
            pltpu.VMEM((768, 768), BF16),
            pltpu.VMEM((768, 768), BF16),
            pltpu.VMEM((560, 128), F32),
            pltpu.VMEM((2, 10, 8, 128), F32),
            pltpu.VMEM((2, 10, 8, 128), F32),
            pltpu.VMEM((2, 72, 128), F32),
            pltpu.VMEM((2, 72, 128), F32),
            pltpu.VMEM((4, 16, 128), F32),
            pltpu.VMEM((4, 16, 128), F32),
            pltpu.VMEM((224, 384), F32),
            pltpu.VMEM((768, 384), F32),
            pltpu.VMEM((count_a, 1, 128), F32),
            pltpu.VMEM((count_b, 1, 128), F32),
            pltpu.VMEM((count_a, 1, 128), F32),
            pltpu.VMEM((count_b, 1, 128), F32),
            pltpu.VMEM((3, 3, 3, 8, 128), F32),
            dma((3,)),
            dma((4,)),
            dma((ROUNDS, 2, 4)),
            dma((ROUNDS, 2, 4)),
            dma((2, 3)),
            dma((2, 8)),
            dma((4, 2, most)),
        ],
        compiler_params=pltpu.CompilerParams(
            collective_id=0, has_side_effects=True, vmem_limit_bytes=48 * 1024 * 1024
        ),
    )

    def on_device(displacement, size_field_modes, velocity):
        adv, grad, checks = call(
            displacement,
            size_field_modes.reshape(27, 4, 128),
            velocity.reshape(3, 4, 128),
            jnp.asarray(wf),
            jnp.asarray(wb),
            jnp.asarray(perm),
            jnp.asarray(cube),
        )
        return adv.reshape(27, 2, 2, 128), grad, checks

    spec = P(None, "gx", "gy", "gz")
    return jax.shard_map(
        on_device, mesh=mesh, in_specs=(spec, spec, spec), out_specs=(spec, spec, P()), check_vma=False
    )
```

```python
import functools

import jax
import jax.numpy as jnp
import numpy as np
from jax import lax
from jax.experimental import pallas as pl
from jax.experimental.pallas import tpu as pltpu
from jax.sharding import PartitionSpec as P

MESH = pl.DeviceIdType.MESH
ROUNDS = 4
C0, C1, C2 = 0.7071067811865476, 1.224744871391589, 1.5811388300841898
ROOT3, ROOT15 = 1.7320508075688772, 3.872983346207417
FACE = C0 * C0 + C1 * C1 + C2 * C2
COURANT = 0.1
THETA = 0.3
OUTER_WEIGHT, INNER_WEIGHT = 0.5 * 0.3478548451374538, 0.5 * 0.6521451548625461
TRIAL = 0.05
F32 = jnp.float32
BF16 = jnp.bfloat16


def tables():
    points = np.array(
        [-0.8611363115940526, -0.3399810435848563, 0.3399810435848563, 0.8611363115940526]
    )
    centred = points
    points = 0.5 * (points + 1.0)
    nodes = np.array([0.0, 1.0 / 3.0, 2.0 / 3.0, 1.0])
    value = np.zeros((4, 4))
    slope = np.zeros((4, 4))
    for column in range(4):
        others = [nodes[m] for m in range(4) if m != column]
        below = np.prod([nodes[column] - m for m in others])
        for row in range(4):
            t = points[row]
            value[row, column] = np.prod([t - m for m in others]) / below
            slope[row, column] = (
                sum(np.prod([t - others[i] for i in range(3) if i != k]) for k in range(3)) / below
            )
    legendre = np.stack(
        [np.full(4, C0), C1 * centred, C2 * 0.5 * (3.0 * centred**2 - 1.0)], axis=1
    )
    wide = np.zeros((2, 2, 3, 4, 4, 4, 4, 7, 8))
    for x in range(2):
        for y in range(2):
            for d in range(3):
                t = [slope if d == axis else value for axis in range(3)]
                wide[x, y, d, :, :, :, :, 3 * x : 3 * x + 4, 3 * y : 3 * y + 4] = np.einsum(
                    "pi,qj,rk->pqrkij", t[0], t[1], t[2]
                )
    wide = wide.reshape(768, 224)
    return legendre, wide


def halves(a):
    hi = np.asarray(a, np.float32).astype(jnp.bfloat16)
    lo = (np.asarray(a, np.float64) - hi.astype(np.float64)).astype(jnp.bfloat16)
    return hi, lo


def split(x):
    hi = x.astype(BF16)
    return hi, (x - hi.astype(F32)).astype(BF16)


def dot(a, b):
    return lax.dot_general(a, b, (((1,), (0,)), ((), ())), preferred_element_type=F32)


def roll(x, by, axis):
    by %= x.shape[axis]
    return x if by == 0 else pltpu.roll(x, by, axis)


def take(ref, d, i):
    return ref[i] if d == 0 else (ref[:, i] if d == 1 else ref[:, :, i])


def kernel(
    nx,
    ny,
    nz,
    disp_any,
    modes_any,
    vel_any,
    wf_any,
    wb_any,
    perm_any,
    adv_any,
    grad_any,
    checks_ref,
    adv_ref,
    grad_ref,
    disp_ref,
    modes_ref,
    vel_ref,
    cube_ref,
    wf_ref,
    wb_ref,
    perm_ref,
    term,
    vel,
    zs_out,
    zs_in,
    face_out,
    face_in,
    diag_out,
    diag_in,
    tx_out,
    tx_in,
    ty_out,
    ty_in,
    td_out,
    td_in,
    din,
    t0,
    t1,
    nf,
    jac,
    s_ref,
    om_ref,
    q_ref,
    gh,
    gl,
    pg,
    gx_out,
    gx_in,
    gy_out,
    gy_in,
    gd_out,
    gd_in,
    nt,
    hh,
    max_a,
    max_b,
    sum_a,
    sum_b,
    max_c,
    sum_c,
    acc_ref,
    local_sem,
    z_sem,
    face_sem,
    diag_sem,
    t_sem,
    g_sem,
    red_sem,
):
    gx, gy, gz = lax.axis_index("gx"), lax.axis_index("gy"), lax.axis_index("gz")

    def at(dx, dy, dz=0):
        return (
            lax.rem(gx + (dx + nx), nx) if dx else gx,
            lax.rem(gy + (dy + ny), ny) if dy else gy,
            lax.rem(gz + (dz + nz), nz) if dz else gz,
        )

    half = nz // 2
    group_a = [
        (i * half + j, (gx, lax.rem(gy + i, ny), lax.rem(gz + 2 * j, nz)))
        for i in range(ny)
        for j in range(half)
        if (i, j) != (0, 0)
    ]
    flipped = gz + 1 - 2 * lax.rem(gz, 2)
    group_b = [
        (i * 2 + b, (lax.rem(gx + 2 * i, nx), gy, flipped if b else gz))
        for i in range(nx // 2)
        for b in range(2)
        if (i, b) != (0, 0)
    ]
    group_c = [(1, (gx + 1 - 2 * lax.rem(gx, 2), gy, gz))]
    count_a, count_b, count_c = ny * half, nx, 2
    corners = ((1, 1), (1, -1), (-1, 1), (-1, -1))
    sides = ((1, 0), (-1, 0), (0, 1), (0, -1))
    partners = [at(*s) for s in sides + corners] + [at(0, 0, 1), at(0, 0, -1)]
    partners += [p for _, p in group_a + group_b + group_c]

    barrier = pltpu.get_barrier_semaphore()
    for p in partners:
        pl.semaphore_signal(barrier, inc=1, device_id=p, device_id_type=MESH)

    loads = [
        pltpu.make_async_copy(a, b, local_sem.at[i])
        for i, (a, b) in enumerate(
            (
                (perm_any, perm_ref),
                (wf_any, wf_ref),
                (wb_any, wb_ref),
                (modes_any, modes_ref),
                (vel_any, vel_ref),
                (disp_any, disp_ref),
            )
        )
    ]
    for i in (3, 4, 5, 0, 1, 2):
        loads[i].start()

    pending = []

    def remote(src, dst, send, recv, to):
        c = pltpu.make_async_remote_copy(
            src_ref=src, dst_ref=dst, send_sem=send, recv_sem=recv, device_id=to, device_id_type=MESH
        )
        c.start()
        pending.append(c)
        return c

    row = lax.broadcasted_iota(jnp.int32, (8, 128), 0)
    lane = lax.broadcasted_iota(jnp.int32, (8, 128), 1)
    xlow = ((row // 2) % 2) == 0
    ylow = (row % 2) == 0
    top = row < 4

    term[0] = jnp.zeros((3, 3, 3, 8, 128), F32)
    vel[...] = jnp.zeros((3, 8, 128), F32)
    point = lax.broadcasted_iota(jnp.int32, (64, 128), 0)
    cube = jnp.ones((64, 128), F32)
    for place in (point // 16, (point // 4) % 4, point % 4):
        cube = cube * jnp.where((place == 0) | (place == 3), OUTER_WEIGHT, INNER_WEIGHT)
    cube_ref[...] = cube
    loads[3].wait()
    loads[4].wait()
    for a in range(3):
        for b in range(3):
            for c in range(3):
                term[0, a, b, c, 0:4, :] = modes_ref[a * 9 + b * 3 + c]
        vel[a, 0:4, :] = vel_ref[a]
    speed = jnp.abs(vel[0]) + jnp.abs(vel[1]) + jnp.abs(vel[2])
    fastest = jnp.max(jnp.max(speed, axis=1, keepdims=True), axis=0, keepdims=True)
    max_a[0] = jnp.broadcast_to(fastest, (1, 128))

    def packed_of(i):
        lo = term[0, (2 * i) // 9, (2 * i) // 3 % 3, (2 * i) % 3] if 2 * i < 27 else vel[2 * i - 27]
        j = 2 * i + 1
        hi = term[0, j // 9, j // 3 % 3, j % 3] if j < 27 else vel[j - 27]
        return jnp.where(top, lo, roll(hi, 4, 0))

    for v in range(2):
        low = jnp.zeros((8, 128), F32)
        high = jnp.zeros((8, 128), F32)
        for i in range(8 * v, min(8 * v + 8, 15)):
            q = i % 8
            w = packed_of(i)
            mine = (lane >= 16 * q) & (lane < 16 * q + 16)
            low = jnp.where(mine, roll(w, 16 * q, 1), low)
            high = jnp.where(mine, roll(w, 16 * q + 16, 1), high)
        zs_out[0, v] = low
        zs_out[1, v] = high

    din[...] = jnp.zeros((144, 384), F32)
    loads[5].wait()
    for c in range(3):
        for x in range(6):
            din[(c * 6 + x) * 8 : (c * 6 + x) * 8 + 6, :] = disp_ref[c, x]
    whole = din[...]
    hi = whole.astype(BF16)
    rest = whole - hi.astype(F32)
    mid = rest.astype(BF16)
    lo = (rest - mid.astype(F32)).astype(BF16)
    loads[0].wait()
    perm = perm_ref[...]
    din[...] = dot(hi, perm) + (dot(mid, perm) + dot(lo, perm))
    t0[...] = jnp.zeros((504, 128), F32)
    low = jnp.zeros((8, 128), F32)
    high = jnp.zeros((8, 128), F32)
    for k in range(3):
        for c in range(3):
            for x in range(6):
                t = k * 3 + c
                j = t * 6 + x
                piece = din[(c * 6 + x) * 8 : (c * 6 + x) * 8 + 8, k * 128 : k * 128 + 128]
                t0[t * 56 + x * 8 : t * 56 + x * 8 + 8, :] = piece
                mine = (lane >= 2 * j) & (lane < 2 * j + 2)
                low = jnp.where(mine, roll(piece, 2 * j, 1), low)
                high = jnp.where(mine, roll(piece, 2 * j + 2, 1), high)
    zs_out[0, 2] = low
    zs_out[1, 2] = high

    pl.semaphore_wait(barrier, len(partners))

    z_up = remote(zs_out.at[1], zs_in.at[1], z_sem.at[0], z_sem.at[1], at(0, 0, 1))
    z_down = remote(zs_out.at[0], zs_in.at[0], z_sem.at[2], z_sem.at[3], at(0, 0, -1))
    maxes_a = [
        remote(max_a.at[0], max_a.at[s], red_sem.at[0, 0, s], red_sem.at[0, 1, s], p)
        for s, p in group_a
    ]
    z_up.wait_recv()
    z_down.wait_recv()
    for v in range(2):
        from_low = zs_in[1, v]
        from_high = zs_in[0, v]
        for i in range(8 * v, min(8 * v + 8, 15)):
            q = i % 8
            near = jnp.where(
                lane < 16,
                roll(from_high, 128 - 16 * q, 1),
                jnp.where(lane >= 112, roll(from_low, 112 - 16 * q, 1), 0.0),
            )
            for j, part in ((2 * i, roll(near, 4, 0)), (2 * i + 1, near)):
                if j < 27:
                    old = term[0, j // 9, j // 3 % 3, j % 3]
                    term[0, j // 9, j // 3 % 3, j % 3] = jnp.where(top, old, part)
                else:
                    vel[j - 27] = jnp.where(top, vel[j - 27], part)

    def zprev(x):
        axis = x.ndim - 1
        r = roll(x, 1, axis)
        return jnp.where(lane == 0, roll(r, 4, axis - 1), r)

    def znext(x):
        axis = x.ndim - 1
        r = roll(x, 127, axis)
        return jnp.where(lane == 127, roll(r, 4, axis - 1), r)

    v0, v1, v2 = vel[0], vel[1], vel[2]
    zero = jnp.zeros((8, 128), F32)
    inner = (
        jnp.where(xlow, 0.0, COURANT * (v0 + roll(v0, 2, 0))),
        jnp.where(ylow, 0.0, COURANT * (v1 + roll(v1, 1, 0))),
        COURANT * (v2 + zprev(v2)),
    )
    plus = [jnp.maximum(f, 0.0) for f in inner]
    minus = [jnp.minimum(f, 0.0) for f in inner]
    grow1 = [(2.0 * COURANT * ROOT3) * v for v in (v0, v1, v2)]
    grow2 = [(2.0 * COURANT * ROOT15) * v for v in (v0, v1, v2)]
    lows = (xlow, ylow)
    signs = (jnp.where(xlow, 1.0, -1.0), jnp.where(ylow, 1.0, -1.0))

    def outward(parts, d):
        e = C0 * parts[0] + C2 * parts[2]
        o = C1 * parts[1]
        return jnp.where(lows[d], e - o, e + o)

    def local_rate(src, dst):
        rims = []
        for d in range(3):
            u0, u1, u2 = take(src, d, 0), take(src, d, 1), take(src, d, 2)
            e = C0 * u0 + C2 * u2
            o = C1 * u1
            tp = e + o
            tm = e - o
            if d < 2:
                rims.append(jnp.where(lows[d], tm, tp))
                by = 2 - d
                lower = plus[d] * roll(tp, by, 2) + minus[d] * tm
                upper = roll(lower, 8 - by, 2)
            else:
                lower = plus[d] * zprev(tp) + minus[d] * tm
                upper = znext(lower)
            drop = lower - upper
            outs = (
                C0 * drop,
                grow1[d] * u0 - C1 * (lower + upper),
                grow2[d] * u1 + C2 * drop,
            )
            for i in range(3):
                if d == 0:
                    dst[i] = outs[i]
                elif d == 1:
                    dst[:, i] = dst[:, i] + outs[i]
                else:
                    dst[:, :, i] = dst[:, :, i] + outs[i]
        return rims

    def add_face(dst, d, flux):
        signed = signs[d] * flux
        outs = (C0 * signed, -C1 * flux, C2 * signed)
        for i in range(3):
            if d == 0:
                dst[i] = dst[i] + outs[i]
            else:
                dst[:, i] = dst[:, i] + outs[i]

    def sides_of(f, d):
        p, m = jnp.maximum(f, 0.0), jnp.minimum(f, 0.0)
        return jnp.where(lows[d], p, m), jnp.where(lows[d], m, p)

    def meet(a, b, d):
        by = 2 - d
        return jnp.where(lows[d], roll(a, 8 - by, a.ndim - 2), roll(b, by, b.ndim - 2))

    corner_rows = (3, 2, 1, 0)

    def pack_corner(values, r):
        tiles = []
        for base in range(0, len(values), 4):
            tile = zero
            for w, value in enumerate(values[base : base + 4]):
                for h in range(2):
                    tile = jnp.where(row == 2 * w + h, roll(value, 2 * w + h - 4 * h - r, 0), tile)
            tiles.append(tile)
        return tiles

    def corner_of(r, w):
        out = zero
        for i, source in enumerate(corner_rows):
            tile = diag_in[r, i, w // 4]
            for h in range(2):
                to = 4 * h + 3 - source
                out = jnp.where(row == to, roll(tile, to - 2 * (w % 4) - h, 0), out)
        return out

    speeds = {}

    def advance(r, hidden):
        src, mid_ref, dst = term.at[2 * r], term.at[2 * r + 1], term.at[2 * r + 2]
        rims = local_rate(src, mid_ref)
        n = 11 if r == 0 else 9
        m = 2 if r == 0 else 1
        for d in range(2):
            by = 2 - d
            far = outward([take(mid_ref, d, i) for i in range(3)], d)
            up = jnp.where(lows[d], roll(far, 8 - by, 2), rims[d])
            down = jnp.where(lows[d], rims[d], roll(far, by, 2))
            for i in range(3):
                face_out[r, 2 * d, 3 * i : 3 * i + 3] = up[i]
                face_out[r, 2 * d + 1, 3 * i : 3 * i + 3] = down[i]
            if r == 0:
                for w in range(2):
                    face_out[r, 2 * d + w, 9] = v0
                    face_out[r, 2 * d + w, 10] = v1
        edge = outward([rims[0][0], rims[0][1], rims[0][2]], 1)
        values = [edge[0], edge[1], edge[2]] + ([v0, v1] if r == 0 else [])
        for i, source in enumerate(corner_rows):
            for w, tile in enumerate(pack_corner(values, source)):
                diag_out[r, i, w] = tile
        corner_copies = [
            remote(
                diag_out.at[r, i, pl.ds(0, m)],
                diag_in.at[r, i, pl.ds(0, m)],
                diag_sem.at[r, 0, i],
                diag_sem.at[r, 1, i],
                at(*s),
            )
            for i, s in enumerate(corners)
        ]
        copies = [
            remote(
                face_out.at[r, i, pl.ds(0, n)],
                face_in.at[r, i, pl.ds(0, n)],
                face_sem.at[r, 0, i],
                face_sem.at[r, 1, i],
                at(*s),
            )
            for i, s in enumerate(sides)
        ]
        hidden()
        for c in copies:
            c.wait_recv()
        if r == 0:
            beside = [meet(face_in[0, 2 * d, 9:11], face_in[0, 2 * d + 1, 9:11], d) for d in (0, 1)]
            speeds["rim"] = (
                sides_of(COURANT * (v0 + beside[0][0]), 0),
                sides_of(COURANT * (v1 + beside[1][1]), 1),
            )
        halves_of = []
        for d in range(2):
            a = face_in[r, 2 * d, 0:9].reshape(3, 3, 8, 128)
            b = face_in[r, 2 * d + 1, 0:9].reshape(3, 3, 8, 128)
            ghost = meet(a, b, d)
            partial = jnp.where(lows[d], a, b)
            theirs, own = speeds["rim"][d]
            flux = theirs * ghost + own * rims[d]
            add_face(mid_ref, d, flux)
            near = outward([ghost[0], ghost[1], ghost[2]], 1 - d)
            halves_of.append((partial - (FACE * signs[d]) * flux, near))
        for c in corner_copies:
            c.wait_recv()
        if r == 0:
            cv0, cv1 = corner_of(0, 3), corner_of(0, 4)
            speeds["far"] = (
                sides_of(COURANT * (beside[0][1] + cv1), 1),
                sides_of(COURANT * (beside[1][0] + cv0), 0),
            )
        edge = jnp.stack([corner_of(r, w) for w in range(3)])
        ghosts = []
        for d in range(2):
            whole_face, near = halves_of[d]
            other = 1 - d
            beyond, inside = speeds["far"][d]
            side_flux = beyond * edge + inside * near
            signed = signs[other] * side_flux
            ghosts.append(
                (
                    whole_face[0] + C0 * signed,
                    whole_face[1] - C1 * side_flux,
                    whole_face[2] + C2 * signed,
                )
            )
        rims = local_rate(mid_ref, dst)
        for d in range(2):
            theirs, own = speeds["rim"][d]
            flux = [theirs * ghosts[d][i] + own * rims[d][i] for i in range(3)]
            for j in range(3):
                signed = signs[d] * flux[j]
                for i, value in enumerate((C0 * signed, -C1 * flux[j], C2 * signed)):
                    if d == 0:
                        dst[i, j] = dst[i, j] + value
                    else:
                        dst[j, i] = dst[j, i] + value

    later = {}

    def hidden0():
        tx_out[9] = zs_in[0, 2]
        tx_out[10] = zs_in[1, 2]
        for t in range(9):
            tx_out[t] = t0[t * 56 : t * 56 + 8, :]
        ty_out[...] = jnp.zeros((80, 128), F32)
        ty_out[0:63, :] = t0[pl.ds(0, 63, stride=8), :]
        td_out[...] = jnp.zeros((32, 128), F32)
        td_out[0:9, :] = t0[pl.ds(0, 9, stride=56), :]
        for out, base in ((ty_out, 64), (td_out, 16)):
            out[base : base + 8, :] = zs_in[0, 2]
            out[base + 8 : base + 16, :] = zs_in[1, 2]
        later["t"] = [
            remote(tx_out, tx_in, t_sem.at[0, 0], t_sem.at[1, 0], at(-1, 0)),
            remote(ty_out, ty_in, t_sem.at[0, 1], t_sem.at[1, 1], at(0, -1)),
            remote(td_out, td_in, t_sem.at[0, 2], t_sem.at[1, 2], at(-1, -1)),
        ]
        for c in maxes_a:
            c.wait_recv()
        best = max_a[0]
        for s in range(1, count_a):
            best = jnp.maximum(best, max_a[s])
        max_c[0] = best
        later["pair"] = [
            remote(max_c.at[0], max_c.at[s], red_sem.at[4, 0, s], red_sem.at[4, 1, s], p)
            for s, p in group_c
        ]

    def hidden1():
        for c in later["pair"]:
            c.wait_recv()
        max_b[0] = jnp.maximum(max_c[0], max_c[1])
        later["max"] = [
            remote(max_b.at[0], max_b.at[s], red_sem.at[1, 0, s], red_sem.at[1, 1, s], p)
            for s, p in group_b
        ]
        for c in later["t"]:
            c.wait_recv()
        for t in range(9):
            t0[t * 56 + 48 : t * 56 + 56, :] = tx_in[t]
        t0[pl.ds(6, 63, stride=8), :] = ty_in[0:63, :]
        t0[pl.ds(54, 9, stride=56), :] = td_in[0:9, :]
        packs = []
        for w in range(2):
            own = jnp.where(
                row < 6, zs_in[w, 2], jnp.where(row == 6, roll(ty_in[64 + 8 * w : 72 + 8 * w, :], 6, 0), 0.0)
            )
            rim = jnp.where(
                row < 6, tx_in[9 + w], jnp.where(row == 6, roll(td_in[16 + 8 * w : 24 + 8 * w, :], 6, 0), 0.0)
            )
            packs.append((own, rim))
        for t in range(9):
            for x in range(7):
                j = t * 6 + x % 6
                from_high, from_low = packs[0][x // 6], packs[1][x // 6]
                t1[t * 56 + x * 8 : t * 56 + x * 8 + 8, :] = jnp.where(
                    lane < 2,
                    roll(from_high, 128 - 2 * j, 1),
                    jnp.where(lane >= 126, roll(from_low, 126 - 2 * j, 1), 0.0),
                )
        wide_lane = lax.broadcasted_iota(jnp.int32, (56, 128), 1)
        for c in range(3):
            for k in range(3):
                t = k * 3 + c
                nf[k * 56 : k * 56 + 56, c * 256 : c * 256 + 128] = t0[t * 56 : t * 56 + 56, :]
                nf[k * 56 : k * 56 + 56, c * 256 + 128 : c * 256 + 256] = t1[t * 56 : t * 56 + 56, :]
            a = roll(t0[c * 56 : c * 56 + 56, :], 127, 1)
            b = roll(t1[c * 56 : c * 56 + 56, :], 127, 1)
            nf[168:224, c * 256 : c * 256 + 128] = jnp.where(wide_lane == 127, b, a)
            nf[168:224, c * 256 + 128 : c * 256 + 256] = jnp.where(wide_lane == 127, a, b)

    def hidden2():
        loads[1].wait()
        for c in range(3):
            a, b = split(nf[:, c * 256 : c * 256 + 256])
            jac[:, c * 256 : c * 256 + 256] = (
                dot(wf_ref[0:768, :], a) + dot(wf_ref[768:1536, :], a) + dot(wf_ref[0:768, :], b)
            )

    series = np.polynomial.polynomial.polypow([1.0, 1.0, 0.5], 4)

    def hidden3():
        for c in later["max"]:
            c.wait_recv()
        best = max_b[0]
        for s in range(1, count_b):
            best = jnp.maximum(best, max_b[s])
        tau = jnp.broadcast_to(1.0 / jnp.maximum(best, 0.25), (8, 128))
        acc = float(series[6]) * term[6]
        for k in range(5, -1, -1):
            acc = acc * tau + float(series[k]) * term[k]
        acc_ref[...] = acc
        tau2 = tau * tau
        tau4 = tau2 * tau2
        later["tau"] = (tau4 * tau2 * tau, tau4 * tau4)
        loads[2].wait()

    for r, hidden in enumerate((hidden0, hidden1, hidden2, hidden3)):
        advance(r, hidden)

    legendre, _ = tables()
    tau7, tau8 = later["tau"]
    field = acc_ref[...] + ((float(series[7]) * tau7) * term[7] + (float(series[8]) * tau8) * term[8])
    acc_ref[...] = field
    for a in range(3):
        for b in range(3):
            for c in range(3):
                adv_ref[a * 9 + b * 3 + c] = field[a, b, c, 0:4]
    leaving = [pltpu.make_async_copy(adv_ref, adv_any, local_sem.at[6])]
    leaving[0].start()
    lg = [[float(v) for v in line] for line in legendre]
    for p in range(4):
        along = lg[p][0] * acc_ref[0] + lg[p][1] * acc_ref[1] + lg[p][2] * acc_ref[2]
        for q in range(4):
            second = lg[q][0] * along[0] + lg[q][1] * along[1] + lg[q][2] * along[2]
            for r in range(4):
                g = p * 16 + q * 4 + r
                s_ref[g * 8 : g * 8 + 8, :] = (
                    lg[r][0] * second[0] + lg[r][1] * second[1] + lg[r][2] * second[2]
                )

    pairs = ((0, 0, 1.0), (1, 1, 1.0), (2, 2, 1.0), (0, 1, 2.0), (0, 2, 2.0), (1, 2, 2.0))

    def jacobian(col, g, tile):
        return [
            [
                jac[pl.ds(pl.multiple_of(col * 192 + d * 64 + g * 16, 16), 16), c * 256 + tile * 128 : c * 256 + tile * 128 + 128]
                + (1.0 if c == d else 0.0)
                for d in range(3)
            ]
            for c in range(3)
        ]

    def strain(jm, q):
        a = {}
        for d, e, _ in pairs:
            k = q * (jm[0][d] * jm[0][e] + jm[1][d] * jm[1][e] + jm[2][d] * jm[2][e])
            a[d, e] = a[e, d] = k - 1.0 if d == e else k
        return a

    def inner_product(a, b):
        on = a[0, 0] * b[0, 0] + a[1, 1] * b[1, 1] + a[2, 2] * b[2, 2]
        off = a[0, 1] * b[0, 1] + a[0, 2] * b[0, 2] + a[1, 2] * b[1, 2]
        return on + 2.0 * off

    def forces(step, energy):
        col, g = step // 4, step % 4
        w = cube_ref[pl.ds(pl.multiple_of(g * 16, 16), 16), :]
        for tile in range(2):
            s = s_ref[pl.ds(g * 128 + tile * 4 + col, 16, stride=8), :]
            size = jnp.exp(THETA * s)
            q = jnp.exp((-2.0 * THETA) * s)
            jm = jacobian(col, g, tile)
            a = strain(jm, q)
            if tile == 0:
                om = w * (size * size * size)
                energy = energy + om * inner_product(a, a)
                at_row = pl.ds(pl.multiple_of(col * 64 + g * 16, 16), 16)
                om_ref[at_row, :] = om
                q_ref[at_row, :] = q
            fac = (4.0 * w) * size
            for d in range(3):
                rows = pl.ds(pl.multiple_of(col * 192 + d * 64 + g * 16, 16), 16)
                for c in range(3):
                    value = fac * (jm[c][0] * a[0, d] + jm[c][1] * a[1, d] + jm[c][2] * a[2, d])
                    hi, lo = split(value)
                    gh[rows, c * 256 + tile * 128 : c * 256 + tile * 128 + 128] = hi
                    gl[rows, c * 256 + tile * 128 : c * 256 + tile * 128 + 128] = lo
        return energy

    energy = lax.fori_loop(0, 16, forces, jnp.zeros((16, 128), F32))

    wide_lane = lax.broadcasted_iota(jnp.int32, (56, 128), 1)
    rim = jnp.zeros((56, 128), F32)
    for c in range(3):
        a = gh[:, c * 256 : c * 256 + 256]
        b = gl[:, c * 256 : c * 256 + 256]
        part = dot(wb_ref[0:224, :], a) + dot(wb_ref[224:448, :], a) + dot(wb_ref[0:224, :], b)
        r0 = roll(part[168:224, 0:128], 1, 1)
        r1 = roll(part[168:224, 128:256], 1, 1)
        pg[c * 56 : c * 56 + 56, :] = part[0:56, 0:128] + jnp.where(wide_lane == 0, r1, r0)
        for k in (1, 2):
            pg[(k * 3 + c) * 56 : (k * 3 + c) * 56 + 56, :] = part[k * 56 : k * 56 + 56, 0:128]
        last = part[0:56, 128:256] + r0
        rim = jnp.where(wide_lane == c, roll(last, c, 1), rim)
    pg[504:560, :] = rim

    for t in range(10):
        gx_out[0, t] = pg[t * 56 + 48 : t * 56 + 56, :]
        gx_out[1, t] = pg[t * 56 : t * 56 + 8, :]
    for i, start in enumerate((54, 48, 6, 0)):
        gd_out[i] = jnp.zeros((16, 128), F32)
        gd_out[i, 0:10, :] = pg[pl.ds(start, 10, stride=56), :]
    for i, start in enumerate((6, 0)):
        gy_out[i] = jnp.zeros((72, 128), F32)
        gy_out[i, 0:70, :] = pg[pl.ds(start, 70, stride=8), :]
    moved = [
        remote(gd_out.at[i], gd_in.at[i], g_sem.at[0, 4 + i], g_sem.at[1, 4 + i], at(*s))
        for i, s in enumerate(corners)
    ]
    moved += [
        remote(gx_out.at[i], gx_in.at[i], g_sem.at[0, i], g_sem.at[1, i], at(*sides[i])) for i in range(2)
    ]
    moved += [
        remote(gy_out.at[i], gy_in.at[i], g_sem.at[0, 2 + i], g_sem.at[1, 2 + i], at(*sides[2 + i]))
        for i in range(2)
    ]
    def total(x):
        return jnp.sum(jnp.sum(x, axis=0, keepdims=True), axis=1, keepdims=True)

    energy = total(energy)
    for c in moved:
        c.wait_recv()
    for t in range(10):
        pg[t * 56 : t * 56 + 8, :] = pg[t * 56 : t * 56 + 8, :] + gx_in[0, t]
        pg[t * 56 + 48 : t * 56 + 56, :] = pg[t * 56 + 48 : t * 56 + 56, :] + gx_in[1, t]
    for i, start in enumerate((0, 6)):
        pg[pl.ds(start, 70, stride=8), :] = pg[pl.ds(start, 70, stride=8), :] + gy_in[i, 0:70, :]
    for i, start in enumerate((0, 6, 48, 54)):
        pg[pl.ds(start, 10, stride=56), :] = pg[pl.ds(start, 10, stride=56), :] + gd_in[i, 0:10, :]

    entries = 81.0 * 512.0 * nx * ny * nz
    own = jnp.zeros((8, 128), F32)
    outer = jnp.zeros((8, 128), F32)
    for t in range(10):
        for x in range(7):
            piece = pg[t * 56 + x * 8 : t * 56 + x * 8 + 8, :]
            if t < 9 and x < 6:
                own = own + piece * piece
            else:
                outer = outer + piece * piece
    square = total(jnp.where(row < 6, own, 0.0))
    reach = total(jnp.where(row < 6, outer, own + outer)) + square
    reach_step = TRIAL / jnp.sqrt(1.0 + reach / entries)

    for c in range(3):
        for k in range(3):
            t = k * 3 + c
            nt[k * 56 : k * 56 + 56, c * 128 : c * 128 + 128] = reach_step * pg[t * 56 : t * 56 + 56, :]
        nt[168:224, c * 128 : c * 128 + 128] = reach_step * jnp.where(
            wide_lane == 127, roll(pg[504:560, :], 127 - c, 1), roll(pg[c * 56 : c * 56 + 56, :], 127, 1)
        )
    a, b = split(nt[...])
    hh[...] = dot(wf_ref[0:768, :], a) + dot(wf_ref[768:1536, :], a) + dot(wf_ref[0:768, :], b)

    def coefficients(step, sums):
        col, g = step // 4, step % 4
        at_row = pl.ds(pl.multiple_of(col * 64 + g * 16, 16), 16)
        om, q = om_ref[at_row, :], q_ref[at_row, :]
        jm = jacobian(col, g, 0)
        hm = [
            [
                hh[pl.ds(pl.multiple_of(col * 192 + d * 64 + g * 16, 16), 16), c * 128 : c * 128 + 128]
                for d in range(3)
            ]
            for c in range(3)
        ]
        a = strain(jm, q)
        b, cc = {}, {}
        for d, e, _ in pairs:
            if d == e:
                k = (2.0 * q) * (jm[0][d] * hm[0][d] + jm[1][d] * hm[1][d] + jm[2][d] * hm[2][d])
            else:
                k = q * (
                    (jm[0][d] * hm[0][e] + jm[1][d] * hm[1][e] + jm[2][d] * hm[2][e])
                    + (jm[0][e] * hm[0][d] + jm[1][e] * hm[1][d] + jm[2][e] * hm[2][d])
                )
            b[d, e] = k
            cc[d, e] = q * (hm[0][d] * hm[0][e] + hm[1][d] * hm[1][e] + hm[2][d] * hm[2][e])
        return (
            sums[0] - om * (2.0 * inner_product(a, b)),
            sums[1] + om * (inner_product(b, b) + 2.0 * inner_product(a, cc)),
            sums[2] - om * (2.0 * inner_product(b, cc)),
            sums[3] + om * inner_product(cc, cc),
        )

    none = jnp.zeros((16, 128), F32)
    sums = lax.fori_loop(0, 16, coefficients, (none, none, none, none))
    line = lax.broadcasted_iota(jnp.int32, (1, 128), 1)
    values = [energy, square, reach_step] + [total(s) for s in sums]
    mine = jnp.zeros((1, 128), F32)
    for i, value in enumerate(values):
        mine = jnp.where(line == i, value, mine)
    sum_a[0] = mine
    sums_a = [
        remote(sum_a.at[0], sum_a.at[s], red_sem.at[2, 0, s], red_sem.at[2, 1, s], p)
        for s, p in group_a
    ]

    for c in range(3):
        for x in range(6):
            for k in range(3):
                t = k * 3 + c
                din[(c * 6 + x) * 8 : (c * 6 + x) * 8 + 8, k * 128 : k * 128 + 128] = pg[
                    t * 56 + x * 8 : t * 56 + x * 8 + 8, :
                ]
    whole = din[...]
    hi = whole.astype(BF16)
    rest = whole - hi.astype(F32)
    mid = rest.astype(BF16)
    lo = (rest - mid.astype(F32)).astype(BF16)
    perm = perm_ref[...]

    def back(x):
        return lax.dot_general(x, perm, (((1,), (1,)), ((), ())), preferred_element_type=F32)

    din[...] = back(hi) + (back(mid) + back(lo))
    for c in range(3):
        for x in range(6):
            grad_ref[c, x] = din[(c * 6 + x) * 8 : (c * 6 + x) * 8 + 6, :]
    leaving.append(pltpu.make_async_copy(grad_ref, grad_any, local_sem.at[7]))
    leaving[1].start()

    def weigh(ratio):
        two = ratio * ratio
        return jnp.where(
            line == 3,
            ratio,
            jnp.where(line == 4, two, jnp.where(line == 5, two * ratio, jnp.where(line == 6, two * two, 1.0))),
        )

    def pick(v, i):
        return jnp.sum(jnp.where(line == i, v, 0.0), axis=1, keepdims=True)

    def combine(ref, count):
        steps = [pick(ref[s], 2) for s in range(count)]
        least = functools.reduce(jnp.minimum, steps)
        out = jnp.zeros((1, 128), F32)
        for s in range(count):
            out = out + ref[s] * weigh(least / steps[s])
        return jnp.where(line == 2, least, out)

    for c in sums_a:
        c.wait_recv()
    sum_c[0] = combine(sum_a, count_a)
    sums_c = [
        remote(sum_c.at[0], sum_c.at[s], red_sem.at[5, 0, s], red_sem.at[5, 1, s], p)
        for s, p in group_c
    ]
    for c in sums_c:
        c.wait_recv()
    sum_b[0] = combine(sum_c, count_c)
    sums_b = [
        remote(sum_b.at[0], sum_b.at[s], red_sem.at[3, 0, s], red_sem.at[3, 1, s], p)
        for s, p in group_b
    ]
    for c in sums_b:
        c.wait_recv()
    final = combine(sum_b, count_b)
    square = pick(final, 1)
    step_length = TRIAL / jnp.sqrt(1.0 + square / entries)
    grown = final * weigh(step_length / pick(final, 2))
    elements = 512.0 * nx * ny * nz
    trial = jnp.sum(jnp.where((line == 0) | ((line >= 3) & (line < 7)), grown, 0.0))
    checks_ref[0] = jnp.sum(jnp.where(line == 0, final, 0.0)) * (1.0 / elements)
    checks_ref[1] = jnp.sum(jnp.where(line == 1, final, 0.0)) * (1.0 / entries)
    checks_ref[2] = trial * (1.0 / elements)

    for c in pending:
        c.wait_send()
    for c in leaving:
        c.wait()


def leave_kernel(a, b, c, to_a, to_b, to_c, sem):
    copies = [
        pltpu.make_async_copy(x, y, sem.at[i]) for i, (x, y) in enumerate(((a, to_a), (b, to_b)))
    ]
    for i in range(3):
        to_c[i] = c[i]
    for copy in copies:
        copy.start()
    for copy in copies:
        copy.wait()


def solution(mesh):
    nx, ny, nz = mesh.shape["gx"], mesh.shape["gy"], mesh.shape["gz"]
    _, wide = tables()
    hi, lo = halves(wide)
    wf = np.concatenate([hi, lo], axis=0)
    wb = np.concatenate([hi.T, lo.T], axis=0)
    perm = np.zeros((384, 384), np.float32)
    for k in range(3):
        perm[3 * np.arange(128) + k, k * 128 + np.arange(128)] = 1.0
    perm = perm.astype(jnp.bfloat16)
    count_a, count_b = ny * (nz // 2), nx
    most = max(count_a, count_b)
    anywhere = pl.BlockSpec(memory_space=pl.ANY)
    hbm = pl.BlockSpec(memory_space=pltpu.HBM)
    dma = pltpu.SemaphoreType.DMA
    call = pl.pallas_call(
        functools.partial(kernel, nx, ny, nz),
        name="tmop_step",
        out_shape=(
            jax.ShapeDtypeStruct((27, 4, 128), F32),
            jax.ShapeDtypeStruct((3, 6, 6, 384), F32),
            jax.ShapeDtypeStruct((3,), F32),
        ),
        in_specs=[hbm] * 6,
        out_specs=(hbm, hbm, pl.BlockSpec(memory_space=pltpu.SMEM)),
        scratch_shapes=[
            pltpu.VMEM((27, 4, 128), F32),
            pltpu.VMEM((3, 6, 6, 384), F32),
            pltpu.VMEM((3, 6, 6, 384), F32),
            pltpu.VMEM((27, 4, 128), F32),
            pltpu.VMEM((3, 4, 128), F32),
            pltpu.VMEM((64, 128), F32),
            pltpu.VMEM((1536, 224), BF16),
            pltpu.VMEM((448, 768), BF16),
            pltpu.VMEM((384, 384), BF16),
            pltpu.VMEM((2 * ROUNDS + 1, 3, 3, 3, 8, 128), F32),
            pltpu.VMEM((3, 8, 128), F32),
            pltpu.VMEM((2, 3, 8, 128), F32),
            pltpu.VMEM((2, 3, 8, 128), F32),
            pltpu.VMEM((ROUNDS, 4, 11, 8, 128), F32),
            pltpu.VMEM((ROUNDS, 4, 11, 8, 128), F32),
            pltpu.VMEM((ROUNDS, 4, 2, 8, 128), F32),
            pltpu.VMEM((ROUNDS, 4, 2, 8, 128), F32),
            pltpu.VMEM((11, 8, 128), F32),
            pltpu.VMEM((11, 8, 128), F32),
            pltpu.VMEM((80, 128), F32),
            pltpu.VMEM((80, 128), F32),
            pltpu.VMEM((32, 128), F32),
            pltpu.VMEM((32, 128), F32),
            pltpu.VMEM((144, 384), F32),
            pltpu.VMEM((504, 128), F32),
            pltpu.VMEM((504, 128), F32),
            pltpu.VMEM((224, 768), F32),
            pltpu.VMEM((768, 768), F32),
            pltpu.VMEM((512, 128), F32),
            pltpu.VMEM((256, 128), F32),
            pltpu.VMEM((256, 128), F32),
            pltpu.VMEM((768, 768), BF16),
            pltpu.VMEM((768, 768), BF16),
            pltpu.VMEM((560, 128), F32),
            pltpu.VMEM((2, 10, 8, 128), F32),
            pltpu.VMEM((2, 10, 8, 128), F32),
            pltpu.VMEM((2, 72, 128), F32),
            pltpu.VMEM((2, 72, 128), F32),
            pltpu.VMEM((4, 16, 128), F32),
            pltpu.VMEM((4, 16, 128), F32),
            pltpu.VMEM((224, 384), F32),
            pltpu.VMEM((768, 384), F32),
            pltpu.VMEM((count_a, 1, 128), F32),
            pltpu.VMEM((count_b, 1, 128), F32),
            pltpu.VMEM((count_a, 1, 128), F32),
            pltpu.VMEM((count_b, 1, 128), F32),
            pltpu.VMEM((2, 1, 128), F32),
            pltpu.VMEM((2, 1, 128), F32),
            pltpu.VMEM((3, 3, 3, 8, 128), F32),
            dma((8,)),
            dma((4,)),
            dma((ROUNDS, 2, 4)),
            dma((ROUNDS, 2, 4)),
            dma((2, 3)),
            dma((2, 8)),
            dma((6, 2, most)),
        ],
        compiler_params=pltpu.CompilerParams(
            collective_id=0, has_side_effects=True, vmem_limit_bytes=67_043_328
        ),
    )

    leave = pl.pallas_call(
        leave_kernel,
        name="leave",
        out_shape=(
            jax.ShapeDtypeStruct((27, 4, 128), F32),
            jax.ShapeDtypeStruct((3, 6, 6, 384), F32),
            jax.ShapeDtypeStruct((3,), F32),
        ),
        in_specs=[pl.BlockSpec(memory_space=pltpu.VMEM)] * 2 + [pl.BlockSpec(memory_space=pltpu.SMEM)],
        out_specs=(hbm,) * 2 + (pl.BlockSpec(memory_space=pltpu.SMEM),),
        scratch_shapes=[dma((2,))],
    )

    def on_device(displacement, size_field_modes, velocity):
        adv, grad, checks = call(
            displacement,
            size_field_modes.reshape(27, 4, 128),
            velocity.reshape(3, 4, 128),
            jnp.asarray(wf),
            jnp.asarray(wb),
            jnp.asarray(perm),
        )
        adv, grad, checks = leave(adv, grad, checks)
        return adv.reshape(27, 2, 2, 128), grad, checks

    spec = P(None, "gx", "gy", "gz")
    return jax.shard_map(
        on_device, mesh=mesh, in_specs=(spec, spec, spec), out_specs=(spec, spec, P()), check_vma=False
    )
```

```python
import functools

import jax
import jax.numpy as jnp
import numpy as np
from jax import lax
from jax.experimental import pallas as pl
from jax.experimental.pallas import tpu as pltpu
from jax.sharding import PartitionSpec as P

MESH = pl.DeviceIdType.MESH
ROUNDS = 4
C0, C1, C2 = 0.7071067811865476, 1.224744871391589, 1.5811388300841898
ROOT3, ROOT15 = 1.7320508075688772, 3.872983346207417
FACE = C0 * C0 + C1 * C1 + C2 * C2
COURANT = 0.1
THETA = 0.3
OUTER_WEIGHT, INNER_WEIGHT = 0.5 * 0.3478548451374538, 0.5 * 0.6521451548625461
TRIAL = 0.05
F32 = jnp.float32
BF16 = jnp.bfloat16


def tables():
    points = np.array(
        [-0.8611363115940526, -0.3399810435848563, 0.3399810435848563, 0.8611363115940526]
    )
    centred = points
    points = 0.5 * (points + 1.0)
    nodes = np.array([0.0, 1.0 / 3.0, 2.0 / 3.0, 1.0])
    value = np.zeros((4, 4))
    slope = np.zeros((4, 4))
    for column in range(4):
        others = [nodes[m] for m in range(4) if m != column]
        below = np.prod([nodes[column] - m for m in others])
        for row in range(4):
            t = points[row]
            value[row, column] = np.prod([t - m for m in others]) / below
            slope[row, column] = (
                sum(np.prod([t - others[i] for i in range(3) if i != k]) for k in range(3)) / below
            )
    legendre = np.stack(
        [np.full(4, C0), C1 * centred, C2 * 0.5 * (3.0 * centred**2 - 1.0)], axis=1
    )
    wide = np.zeros((2, 2, 3, 4, 4, 4, 4, 7, 8))
    for x in range(2):
        for y in range(2):
            for d in range(3):
                t = [slope if d == axis else value for axis in range(3)]
                wide[x, y, d, :, :, :, :, 3 * x : 3 * x + 4, 3 * y : 3 * y + 4] = np.einsum(
                    "pi,qj,rk->pqrkij", t[0], t[1], t[2]
                )
    wide = wide.reshape(768, 224)
    return legendre, wide


def halves(a):
    hi = np.asarray(a, np.float32).astype(jnp.bfloat16)
    lo = (np.asarray(a, np.float64) - hi.astype(np.float64)).astype(jnp.bfloat16)
    return hi, lo


def split(x):
    hi = x.astype(BF16)
    return hi, (x - hi.astype(F32)).astype(BF16)


def dot(a, b):
    return lax.dot_general(a, b, (((1,), (0,)), ((), ())), preferred_element_type=F32)


def roll(x, by, axis):
    by %= x.shape[axis]
    return x if by == 0 else pltpu.roll(x, by, axis)


def take(ref, d, i):
    return ref[i] if d == 0 else (ref[:, i] if d == 1 else ref[:, :, i])


def kernel(
    nx,
    ny,
    nz,
    disp_any,
    modes_any,
    vel_any,
    wf_any,
    wb_any,
    perm_any,
    adv_any,
    grad_any,
    checks_ref,
    adv_ref,
    grad_ref,
    disp_ref,
    modes_ref,
    vel_ref,
    cube_ref,
    wf_ref,
    wb_ref,
    perm_ref,
    term,
    vel,
    zs_out,
    zs_in,
    face_out,
    face_in,
    diag_out,
    diag_in,
    tx_out,
    tx_in,
    ty_out,
    ty_in,
    td_out,
    td_in,
    din,
    t0,
    t1,
    nf,
    jac,
    s_ref,
    om_ref,
    q_ref,
    gh,
    gl,
    pg,
    gx_out,
    gx_in,
    gy_out,
    gy_in,
    gd_out,
    gd_in,
    nt,
    hh,
    max_a,
    max_b,
    sum_a,
    sum_b,
    max_c,
    sum_c,
    acc_ref,
    local_sem,
    z_sem,
    face_sem,
    diag_sem,
    t_sem,
    g_sem,
    red_sem,
):
    gx, gy, gz = lax.axis_index("gx"), lax.axis_index("gy"), lax.axis_index("gz")

    def at(dx, dy, dz=0):
        return (
            lax.rem(gx + (dx + nx), nx) if dx else gx,
            lax.rem(gy + (dy + ny), ny) if dy else gy,
            lax.rem(gz + (dz + nz), nz) if dz else gz,
        )

    half = nz // 2
    group_a = [
        (i * half + j, (gx, lax.rem(gy + i, ny), lax.rem(gz + 2 * j, nz)))
        for i in range(ny)
        for j in range(half)
        if (i, j) != (0, 0)
    ]
    flipped = gz + 1 - 2 * lax.rem(gz, 2)
    group_b = [
        (i * 2 + b, (lax.rem(gx + 2 * i, nx), gy, flipped if b else gz))
        for i in range(nx // 2)
        for b in range(2)
        if (i, b) != (0, 0)
    ]
    group_c = [(1, (gx + 1 - 2 * lax.rem(gx, 2), gy, gz))]
    count_a, count_b, count_c = ny * half, nx, 2
    corners = ((1, 1), (1, -1), (-1, 1), (-1, -1))
    sides = ((1, 0), (-1, 0), (0, 1), (0, -1))
    partners = [at(*s) for s in sides + corners] + [at(0, 0, 1), at(0, 0, -1)]
    partners += [p for _, p in group_a + group_b + group_c]

    barrier = pltpu.get_barrier_semaphore()
    for p in partners:
        pl.semaphore_signal(barrier, inc=1, device_id=p, device_id_type=MESH)

    loads = [
        pltpu.make_async_copy(a, b, local_sem.at[i])
        for i, (a, b) in enumerate(
            (
                (perm_any, perm_ref),
                (wf_any, wf_ref),
                (wb_any, wb_ref),
                (modes_any, modes_ref),
                (vel_any, vel_ref),
                (disp_any, disp_ref),
            )
        )
    ]
    for i in (3, 4, 5, 0, 1, 2):
        loads[i].start()

    pending = []

    def remote(src, dst, send, recv, to):
        c = pltpu.make_async_remote_copy(
            src_ref=src, dst_ref=dst, send_sem=send, recv_sem=recv, device_id=to, device_id_type=MESH
        )
        c.start()
        pending.append(c)
        return c

    row = lax.broadcasted_iota(jnp.int32, (8, 128), 0)
    lane = lax.broadcasted_iota(jnp.int32, (8, 128), 1)
    xlow = ((row // 2) % 2) == 0
    ylow = (row % 2) == 0
    top = row < 4

    term[0] = jnp.zeros((3, 3, 3, 8, 128), F32)
    vel[...] = jnp.zeros((3, 8, 128), F32)
    point = lax.broadcasted_iota(jnp.int32, (64, 128), 0)
    cube = jnp.ones((64, 128), F32)
    for place in (point // 16, (point // 4) % 4, point % 4):
        cube = cube * jnp.where((place == 0) | (place == 3), OUTER_WEIGHT, INNER_WEIGHT)
    cube_ref[...] = cube
    loads[3].wait()
    loads[4].wait()
    for a in range(3):
        for b in range(3):
            for c in range(3):
                term[0, a, b, c, 0:4, :] = modes_ref[a * 9 + b * 3 + c]
        vel[a, 0:4, :] = vel_ref[a]
    speed = jnp.abs(vel[0]) + jnp.abs(vel[1]) + jnp.abs(vel[2])
    fastest = jnp.max(jnp.max(speed, axis=1, keepdims=True), axis=0, keepdims=True)
    max_a[0] = jnp.broadcast_to(fastest, (1, 128))

    def packed_of(i):
        lo = term[0, (2 * i) // 9, (2 * i) // 3 % 3, (2 * i) % 3] if 2 * i < 27 else vel[2 * i - 27]
        j = 2 * i + 1
        hi = term[0, j // 9, j // 3 % 3, j % 3] if j < 27 else vel[j - 27]
        return jnp.where(top, lo, roll(hi, 4, 0))

    for v in range(2):
        low = jnp.zeros((8, 128), F32)
        high = jnp.zeros((8, 128), F32)
        for i in range(8 * v, min(8 * v + 8, 15)):
            q = i % 8
            w = packed_of(i)
            mine = (lane >= 16 * q) & (lane < 16 * q + 16)
            low = jnp.where(mine, roll(w, 16 * q, 1), low)
            high = jnp.where(mine, roll(w, 16 * q + 16, 1), high)
        zs_out[0, v] = low
        zs_out[1, v] = high

    pl.semaphore_wait(barrier, len(partners))

    def along_z(part, base):
        return [
            remote(
                zs_out.at[w, part], zs_in.at[w, part], z_sem.at[base + w], z_sem.at[base + 2 + w], at(0, 0, to)
            )
            for w, to in ((1, 1), (0, -1))
        ]

    z_field = along_z(pl.ds(0, 2), 0)
    maxes_a = [
        remote(max_a.at[0], max_a.at[s], red_sem.at[0, 0, s], red_sem.at[0, 1, s], p)
        for s, p in group_a
    ]
    din[...] = jnp.zeros((144, 384), F32)
    loads[5].wait()
    for c in range(3):
        for x in range(6):
            din[(c * 6 + x) * 8 : (c * 6 + x) * 8 + 6, :] = disp_ref[c, x]
    whole = din[...]
    hi = whole.astype(BF16)
    rest = whole - hi.astype(F32)
    mid = rest.astype(BF16)
    lo = (rest - mid.astype(F32)).astype(BF16)
    loads[0].wait()
    perm = perm_ref[...]
    din[...] = dot(hi, perm) + (dot(mid, perm) + dot(lo, perm))
    t0[...] = jnp.zeros((504, 128), F32)
    low = jnp.zeros((8, 128), F32)
    high = jnp.zeros((8, 128), F32)
    for k in range(3):
        for c in range(3):
            for x in range(6):
                t = k * 3 + c
                j = t * 6 + x
                piece = din[(c * 6 + x) * 8 : (c * 6 + x) * 8 + 8, k * 128 : k * 128 + 128]
                t0[t * 56 + x * 8 : t * 56 + x * 8 + 8, :] = piece
                mine = (lane >= 2 * j) & (lane < 2 * j + 2)
                low = jnp.where(mine, roll(piece, 2 * j, 1), low)
                high = jnp.where(mine, roll(piece, 2 * j + 2, 1), high)
    zs_out[0, 2] = low
    zs_out[1, 2] = high

    z_nodes = along_z(pl.ds(2, 1), 4)
    for c in z_field:
        c.wait_recv()
    for v in range(2):
        from_low = zs_in[1, v]
        from_high = zs_in[0, v]
        for i in range(8 * v, min(8 * v + 8, 15)):
            q = i % 8
            near = jnp.where(
                lane < 16,
                roll(from_high, 128 - 16 * q, 1),
                jnp.where(lane >= 112, roll(from_low, 112 - 16 * q, 1), 0.0),
            )
            for j, part in ((2 * i, roll(near, 4, 0)), (2 * i + 1, near)):
                if j < 27:
                    old = term[0, j // 9, j // 3 % 3, j % 3]
                    term[0, j // 9, j // 3 % 3, j % 3] = jnp.where(top, old, part)
                else:
                    vel[j - 27] = jnp.where(top, vel[j - 27], part)

    def zprev(x):
        axis = x.ndim - 1
        r = roll(x, 1, axis)
        return jnp.where(lane == 0, roll(r, 4, axis - 1), r)

    def znext(x):
        axis = x.ndim - 1
        r = roll(x, 127, axis)
        return jnp.where(lane == 127, roll(r, 4, axis - 1), r)

    v0, v1, v2 = vel[0], vel[1], vel[2]
    zero = jnp.zeros((8, 128), F32)
    inner = (
        jnp.where(xlow, 0.0, COURANT * (v0 + roll(v0, 2, 0))),
        jnp.where(ylow, 0.0, COURANT * (v1 + roll(v1, 1, 0))),
        COURANT * (v2 + zprev(v2)),
    )
    plus = [jnp.maximum(f, 0.0) for f in inner]
    minus = [jnp.minimum(f, 0.0) for f in inner]
    grow1 = [(2.0 * COURANT * ROOT3) * v for v in (v0, v1, v2)]
    grow2 = [(2.0 * COURANT * ROOT15) * v for v in (v0, v1, v2)]
    lows = (xlow, ylow)
    signs = (jnp.where(xlow, 1.0, -1.0), jnp.where(ylow, 1.0, -1.0))

    def outward(parts, d):
        e = C0 * parts[0] + C2 * parts[2]
        o = C1 * parts[1]
        return jnp.where(lows[d], e - o, e + o)

    def local_rate(src, dst):
        rims = []
        for d in range(3):
            u0, u1, u2 = take(src, d, 0), take(src, d, 1), take(src, d, 2)
            e = C0 * u0 + C2 * u2
            o = C1 * u1
            tp = e + o
            tm = e - o
            if d < 2:
                rims.append(jnp.where(lows[d], tm, tp))
                by = 2 - d
                lower = plus[d] * roll(tp, by, 2) + minus[d] * tm
                upper = roll(lower, 8 - by, 2)
            else:
                lower = plus[d] * zprev(tp) + minus[d] * tm
                upper = znext(lower)
            drop = lower - upper
            outs = (
                C0 * drop,
                grow1[d] * u0 - C1 * (lower + upper),
                grow2[d] * u1 + C2 * drop,
            )
            for i in range(3):
                if d == 0:
                    dst[i] = outs[i]
                elif d == 1:
                    dst[:, i] = dst[:, i] + outs[i]
                else:
                    dst[:, :, i] = dst[:, :, i] + outs[i]
        return rims

    def add_face(dst, d, flux):
        signed = signs[d] * flux
        outs = (C0 * signed, -C1 * flux, C2 * signed)
        for i in range(3):
            if d == 0:
                dst[i] = dst[i] + outs[i]
            else:
                dst[:, i] = dst[:, i] + outs[i]

    def sides_of(f, d):
        p, m = jnp.maximum(f, 0.0), jnp.minimum(f, 0.0)
        return jnp.where(lows[d], p, m), jnp.where(lows[d], m, p)

    def meet(a, b, d):
        by = 2 - d
        return jnp.where(lows[d], roll(a, 8 - by, a.ndim - 2), roll(b, by, b.ndim - 2))

    corner_rows = (3, 2, 1, 0)

    def pack_corner(values, r):
        tiles = []
        for base in range(0, len(values), 4):
            tile = zero
            for w, value in enumerate(values[base : base + 4]):
                for h in range(2):
                    tile = jnp.where(row == 2 * w + h, roll(value, 2 * w + h - 4 * h - r, 0), tile)
            tiles.append(tile)
        return tiles

    def corner_of(r, w):
        out = zero
        for i, source in enumerate(corner_rows):
            tile = diag_in[r, i, w // 4]
            for h in range(2):
                to = 4 * h + 3 - source
                out = jnp.where(row == to, roll(tile, to - 2 * (w % 4) - h, 0), out)
        return out

    speeds = {}

    def advance(r, hidden):
        src, mid_ref, dst = term.at[2 * r], term.at[2 * r + 1], term.at[2 * r + 2]
        m = 2 if r == 0 else 1
        first = outward([take(src, 0, i) for i in range(3)], 0)
        edge = outward([first[0], first[1], first[2]], 1)
        values = [edge[0], edge[1], edge[2]] + ([v0, v1] if r == 0 else [])
        for i, source in enumerate(corner_rows):
            for w, tile in enumerate(pack_corner(values, source)):
                diag_out[r, i, w] = tile
        corner_copies = [
            remote(
                diag_out.at[r, i, pl.ds(0, m)],
                diag_in.at[r, i, pl.ds(0, m)],
                diag_sem.at[r, 0, i],
                diag_sem.at[r, 1, i],
                at(*s),
            )
            for i, s in enumerate(corners)
        ]
        rims = local_rate(src, mid_ref)
        n = 11 if r == 0 else 9
        for d in range(2):
            by = 2 - d
            far = outward([take(mid_ref, d, i) for i in range(3)], d)
            up = jnp.where(lows[d], roll(far, 8 - by, 2), rims[d])
            down = jnp.where(lows[d], rims[d], roll(far, by, 2))
            for i in range(3):
                face_out[r, 2 * d, 3 * i : 3 * i + 3] = up[i]
                face_out[r, 2 * d + 1, 3 * i : 3 * i + 3] = down[i]
            if r == 0:
                for w in range(2):
                    face_out[r, 2 * d + w, 9] = v0
                    face_out[r, 2 * d + w, 10] = v1
        copies = [
            remote(
                face_out.at[r, i, pl.ds(0, n)],
                face_in.at[r, i, pl.ds(0, n)],
                face_sem.at[r, 0, i],
                face_sem.at[r, 1, i],
                at(*s),
            )
            for i, s in enumerate(sides)
        ]
        hidden()
        for c in copies:
            c.wait_recv()
        if r == 0:
            beside = [meet(face_in[0, 2 * d, 9:11], face_in[0, 2 * d + 1, 9:11], d) for d in (0, 1)]
            speeds["rim"] = (
                sides_of(COURANT * (v0 + beside[0][0]), 0),
                sides_of(COURANT * (v1 + beside[1][1]), 1),
            )
        halves_of = []
        for d in range(2):
            a = face_in[r, 2 * d, 0:9].reshape(3, 3, 8, 128)
            b = face_in[r, 2 * d + 1, 0:9].reshape(3, 3, 8, 128)
            ghost = meet(a, b, d)
            partial = jnp.where(lows[d], a, b)
            theirs, own = speeds["rim"][d]
            flux = theirs * ghost + own * rims[d]
            add_face(mid_ref, d, flux)
            near = outward([ghost[0], ghost[1], ghost[2]], 1 - d)
            halves_of.append((partial - (FACE * signs[d]) * flux, near))
        for c in corner_copies:
            c.wait_recv()
        if r == 0:
            cv0, cv1 = corner_of(0, 3), corner_of(0, 4)
            speeds["far"] = (
                sides_of(COURANT * (beside[0][1] + cv1), 1),
                sides_of(COURANT * (beside[1][0] + cv0), 0),
            )
        edge = jnp.stack([corner_of(r, w) for w in range(3)])
        ghosts = []
        for d in range(2):
            whole_face, near = halves_of[d]
            other = 1 - d
            beyond, inside = speeds["far"][d]
            side_flux = beyond * edge + inside * near
            signed = signs[other] * side_flux
            ghosts.append(
                (
                    whole_face[0] + C0 * signed,
                    whole_face[1] - C1 * side_flux,
                    whole_face[2] + C2 * signed,
                )
            )
        rims = local_rate(mid_ref, dst)
        for d in range(2):
            theirs, own = speeds["rim"][d]
            flux = [theirs * ghosts[d][i] + own * rims[d][i] for i in range(3)]
            for j in range(3):
                signed = signs[d] * flux[j]
                for i, value in enumerate((C0 * signed, -C1 * flux[j], C2 * signed)):
                    if d == 0:
                        dst[i, j] = dst[i, j] + value
                    else:
                        dst[j, i] = dst[j, i] + value

    later = {}

    def hidden0():
        for c in maxes_a:
            c.wait_recv()
        best = max_a[0]
        for s in range(1, count_a):
            best = jnp.maximum(best, max_a[s])
        max_c[0] = best
        later["pair"] = [
            remote(max_c.at[0], max_c.at[s], red_sem.at[4, 0, s], red_sem.at[4, 1, s], p)
            for s, p in group_c
        ]

    def hidden1():
        for c in later["pair"]:
            c.wait_recv()
        max_b[0] = jnp.maximum(max_c[0], max_c[1])
        later["max"] = [
            remote(max_b.at[0], max_b.at[s], red_sem.at[1, 0, s], red_sem.at[1, 1, s], p)
            for s, p in group_b
        ]
        for c in z_nodes:
            c.wait_recv()
        tx_out[9] = zs_in[0, 2]
        tx_out[10] = zs_in[1, 2]
        for t in range(9):
            tx_out[t] = t0[t * 56 : t * 56 + 8, :]
        ty_out[...] = jnp.zeros((80, 128), F32)
        ty_out[0:63, :] = t0[pl.ds(0, 63, stride=8), :]
        td_out[...] = jnp.zeros((32, 128), F32)
        td_out[0:9, :] = t0[pl.ds(0, 9, stride=56), :]
        for out, base in ((ty_out, 64), (td_out, 16)):
            out[base : base + 8, :] = zs_in[0, 2]
            out[base + 8 : base + 16, :] = zs_in[1, 2]
        later["t"] = [
            remote(tx_out, tx_in, t_sem.at[0, 0], t_sem.at[1, 0], at(-1, 0)),
            remote(ty_out, ty_in, t_sem.at[0, 1], t_sem.at[1, 1], at(0, -1)),
            remote(td_out, td_in, t_sem.at[0, 2], t_sem.at[1, 2], at(-1, -1)),
        ]

    def hidden2():
        for c in later["t"]:
            c.wait_recv()
        for t in range(9):
            t0[t * 56 + 48 : t * 56 + 56, :] = tx_in[t]
        t0[pl.ds(6, 63, stride=8), :] = ty_in[0:63, :]
        t0[pl.ds(54, 9, stride=56), :] = td_in[0:9, :]
        packs = []
        for w in range(2):
            own = jnp.where(
                row < 6, zs_in[w, 2], jnp.where(row == 6, roll(ty_in[64 + 8 * w : 72 + 8 * w, :], 6, 0), 0.0)
            )
            rim = jnp.where(
                row < 6, tx_in[9 + w], jnp.where(row == 6, roll(td_in[16 + 8 * w : 24 + 8 * w, :], 6, 0), 0.0)
            )
            packs.append((own, rim))
        for t in range(9):
            for x in range(7):
                j = t * 6 + x % 6
                from_high, from_low = packs[0][x // 6], packs[1][x // 6]
                t1[t * 56 + x * 8 : t * 56 + x * 8 + 8, :] = jnp.where(
                    lane < 2,
                    roll(from_high, 128 - 2 * j, 1),
                    jnp.where(lane >= 126, roll(from_low, 126 - 2 * j, 1), 0.0),
                )
        wide_lane = lax.broadcasted_iota(jnp.int32, (56, 128), 1)
        for c in range(3):
            for k in range(3):
                t = k * 3 + c
                nf[k * 56 : k * 56 + 56, c * 256 : c * 256 + 128] = t0[t * 56 : t * 56 + 56, :]
                nf[k * 56 : k * 56 + 56, c * 256 + 128 : c * 256 + 256] = t1[t * 56 : t * 56 + 56, :]
            a = roll(t0[c * 56 : c * 56 + 56, :], 127, 1)
            b = roll(t1[c * 56 : c * 56 + 56, :], 127, 1)
            nf[168:224, c * 256 : c * 256 + 128] = jnp.where(wide_lane == 127, b, a)
            nf[168:224, c * 256 + 128 : c * 256 + 256] = jnp.where(wide_lane == 127, a, b)

        loads[1].wait()
        for c in range(3):
            a, b = split(nf[:, c * 256 : c * 256 + 256])
            jac[:, c * 256 : c * 256 + 256] = (
                dot(wf_ref[0:768, :], a) + dot(wf_ref[768:1536, :], a) + dot(wf_ref[0:768, :], b)
            )

    series = np.polynomial.polynomial.polypow([1.0, 1.0, 0.5], 4)

    def hidden3():
        for c in later["max"]:
            c.wait_recv()
        best = max_b[0]
        for s in range(1, count_b):
            best = jnp.maximum(best, max_b[s])
        tau = jnp.broadcast_to(1.0 / jnp.maximum(best, 0.25), (8, 128))
        acc = float(series[6]) * term[6]
        for k in range(5, -1, -1):
            acc = acc * tau + float(series[k]) * term[k]
        acc_ref[...] = acc
        tau2 = tau * tau
        tau4 = tau2 * tau2
        later["tau"] = (tau4 * tau2 * tau, tau4 * tau4)
        loads[2].wait()

    for r, hidden in enumerate((hidden0, hidden1, hidden2, hidden3)):
        advance(r, hidden)

    legendre, _ = tables()
    tau7, tau8 = later["tau"]
    field = acc_ref[...] + ((float(series[7]) * tau7) * term[7] + (float(series[8]) * tau8) * term[8])
    acc_ref[...] = field
    for a in range(3):
        for b in range(3):
            for c in range(3):
                adv_ref[a * 9 + b * 3 + c] = field[a, b, c, 0:4]
    leaving = [pltpu.make_async_copy(adv_ref, adv_any, local_sem.at[6])]
    leaving[0].start()
    lg = [[float(v) for v in line] for line in legendre]
    for p in range(4):
        along = lg[p][0] * acc_ref[0] + lg[p][1] * acc_ref[1] + lg[p][2] * acc_ref[2]
        for q in range(4):
            second = lg[q][0] * along[0] + lg[q][1] * along[1] + lg[q][2] * along[2]
            for r in range(4):
                g = p * 16 + q * 4 + r
                s_ref[g * 8 : g * 8 + 8, :] = (
                    lg[r][0] * second[0] + lg[r][1] * second[1] + lg[r][2] * second[2]
                )

    pairs = ((0, 0, 1.0), (1, 1, 1.0), (2, 2, 1.0), (0, 1, 2.0), (0, 2, 2.0), (1, 2, 2.0))

    def jacobian(col, g, tile):
        return [
            [
                jac[pl.ds(pl.multiple_of(col * 192 + d * 64 + g * 16, 16), 16), c * 256 + tile * 128 : c * 256 + tile * 128 + 128]
                + (1.0 if c == d else 0.0)
                for d in range(3)
            ]
            for c in range(3)
        ]

    def strain(jm, q):
        a = {}
        for d, e, _ in pairs:
            k = q * (jm[0][d] * jm[0][e] + jm[1][d] * jm[1][e] + jm[2][d] * jm[2][e])
            a[d, e] = a[e, d] = k - 1.0 if d == e else k
        return a

    def inner_product(a, b):
        on = a[0, 0] * b[0, 0] + a[1, 1] * b[1, 1] + a[2, 2] * b[2, 2]
        off = a[0, 1] * b[0, 1] + a[0, 2] * b[0, 2] + a[1, 2] * b[1, 2]
        return on + 2.0 * off

    def forces(step, energy):
        col, g = step // 4, step % 4
        w = cube_ref[pl.ds(pl.multiple_of(g * 16, 16), 16), :]
        for tile in range(2):
            s = s_ref[pl.ds(g * 128 + tile * 4 + col, 16, stride=8), :]
            size = jnp.exp(THETA * s)
            q = jnp.exp((-2.0 * THETA) * s)
            jm = jacobian(col, g, tile)
            a = strain(jm, q)
            if tile == 0:
                om = w * (size * size * size)
                energy = energy + om * inner_product(a, a)
                at_row = pl.ds(pl.multiple_of(col * 64 + g * 16, 16), 16)
                om_ref[at_row, :] = om
                q_ref[at_row, :] = q
            fac = (4.0 * w) * size
            for d in range(3):
                rows = pl.ds(pl.multiple_of(col * 192 + d * 64 + g * 16, 16), 16)
                for c in range(3):
                    value = fac * (jm[c][0] * a[0, d] + jm[c][1] * a[1, d] + jm[c][2] * a[2, d])
                    hi, lo = split(value)
                    gh[rows, c * 256 + tile * 128 : c * 256 + tile * 128 + 128] = hi
                    gl[rows, c * 256 + tile * 128 : c * 256 + tile * 128 + 128] = lo
        return energy

    energy = lax.fori_loop(0, 16, forces, jnp.zeros((16, 128), F32), unroll=2)

    wide_lane = lax.broadcasted_iota(jnp.int32, (56, 128), 1)
    rim = jnp.zeros((56, 128), F32)
    for c in range(3):
        a = gh[:, c * 256 : c * 256 + 256]
        b = gl[:, c * 256 : c * 256 + 256]
        both = dot(wb_ref[...], a)
        part = both[0:224, :] + both[224:448, :] + dot(wb_ref[0:224, :], b)
        r0 = roll(part[168:224, 0:128], 1, 1)
        r1 = roll(part[168:224, 128:256], 1, 1)
        pg[c * 56 : c * 56 + 56, :] = part[0:56, 0:128] + jnp.where(wide_lane == 0, r1, r0)
        for k in (1, 2):
            pg[(k * 3 + c) * 56 : (k * 3 + c) * 56 + 56, :] = part[k * 56 : k * 56 + 56, 0:128]
        last = part[0:56, 128:256] + r0
        rim = jnp.where(wide_lane == c, roll(last, c, 1), rim)
    pg[504:560, :] = rim

    for t in range(10):
        gx_out[0, t] = pg[t * 56 + 48 : t * 56 + 56, :]
        gx_out[1, t] = pg[t * 56 : t * 56 + 8, :]
    for i, start in enumerate((54, 48, 6, 0)):
        gd_out[i] = jnp.zeros((16, 128), F32)
        gd_out[i, 0:10, :] = pg[pl.ds(start, 10, stride=56), :]
    for i, start in enumerate((6, 0)):
        gy_out[i] = jnp.zeros((72, 128), F32)
        gy_out[i, 0:70, :] = pg[pl.ds(start, 70, stride=8), :]
    moved = [
        remote(gd_out.at[i], gd_in.at[i], g_sem.at[0, 4 + i], g_sem.at[1, 4 + i], at(*s))
        for i, s in enumerate(corners)
    ]
    moved += [
        remote(gx_out.at[i], gx_in.at[i], g_sem.at[0, i], g_sem.at[1, i], at(*sides[i])) for i in range(2)
    ]
    moved += [
        remote(gy_out.at[i], gy_in.at[i], g_sem.at[0, 2 + i], g_sem.at[1, 2 + i], at(*sides[2 + i]))
        for i in range(2)
    ]
    def total(x):
        return jnp.sum(jnp.sum(x, axis=0, keepdims=True), axis=1, keepdims=True)

    energy = total(energy)
    for c in moved:
        c.wait_recv()
    for t in range(10):
        pg[t * 56 : t * 56 + 8, :] = pg[t * 56 : t * 56 + 8, :] + gx_in[0, t]
        pg[t * 56 + 48 : t * 56 + 56, :] = pg[t * 56 + 48 : t * 56 + 56, :] + gx_in[1, t]
    for i, start in enumerate((0, 6)):
        pg[pl.ds(start, 70, stride=8), :] = pg[pl.ds(start, 70, stride=8), :] + gy_in[i, 0:70, :]
    for i, start in enumerate((0, 6, 48, 54)):
        pg[pl.ds(start, 10, stride=56), :] = pg[pl.ds(start, 10, stride=56), :] + gd_in[i, 0:10, :]

    entries = 81.0 * 512.0 * nx * ny * nz
    own = jnp.zeros((8, 128), F32)
    outer = jnp.zeros((8, 128), F32)
    for t in range(10):
        for x in range(7):
            piece = pg[t * 56 + x * 8 : t * 56 + x * 8 + 8, :]
            if t < 9 and x < 6:
                own = own + piece * piece
            else:
                outer = outer + piece * piece
    square = total(jnp.where(row < 6, own, 0.0))
    reach = total(jnp.where(row < 6, outer, own + outer)) + square
    reach_step = TRIAL / jnp.sqrt(1.0 + reach / entries)

    for c in range(3):
        for k in range(3):
            t = k * 3 + c
            nt[k * 56 : k * 56 + 56, c * 128 : c * 128 + 128] = reach_step * pg[t * 56 : t * 56 + 56, :]
        nt[168:224, c * 128 : c * 128 + 128] = reach_step * jnp.where(
            wide_lane == 127, roll(pg[504:560, :], 127 - c, 1), roll(pg[c * 56 : c * 56 + 56, :], 127, 1)
        )
    a, b = split(nt[...])
    both = dot(wf_ref[...], a)
    hh[...] = both[0:768, :] + both[768:1536, :] + dot(wf_ref[0:768, :], b)

    def coefficients(step, sums):
        col, g = step // 4, step % 4
        at_row = pl.ds(pl.multiple_of(col * 64 + g * 16, 16), 16)
        om, q = om_ref[at_row, :], q_ref[at_row, :]
        jm = jacobian(col, g, 0)
        hm = [
            [
                hh[pl.ds(pl.multiple_of(col * 192 + d * 64 + g * 16, 16), 16), c * 128 : c * 128 + 128]
                for d in range(3)
            ]
            for c in range(3)
        ]
        a = strain(jm, q)
        b, cc = {}, {}
        for d, e, _ in pairs:
            if d == e:
                k = (2.0 * q) * (jm[0][d] * hm[0][d] + jm[1][d] * hm[1][d] + jm[2][d] * hm[2][d])
            else:
                k = q * (
                    (jm[0][d] * hm[0][e] + jm[1][d] * hm[1][e] + jm[2][d] * hm[2][e])
                    + (jm[0][e] * hm[0][d] + jm[1][e] * hm[1][d] + jm[2][e] * hm[2][d])
                )
            b[d, e] = k
            cc[d, e] = q * (hm[0][d] * hm[0][e] + hm[1][d] * hm[1][e] + hm[2][d] * hm[2][e])
        return (
            sums[0] - om * (2.0 * inner_product(a, b)),
            sums[1] + om * (inner_product(b, b) + 2.0 * inner_product(a, cc)),
            sums[2] - om * (2.0 * inner_product(b, cc)),
            sums[3] + om * inner_product(cc, cc),
        )

    none = jnp.zeros((16, 128), F32)
    sums = lax.fori_loop(0, 16, coefficients, (none, none, none, none), unroll=2)
    line = lax.broadcasted_iota(jnp.int32, (1, 128), 1)
    values = [energy, square, reach_step] + [total(s) for s in sums]
    mine = jnp.zeros((1, 128), F32)
    for i, value in enumerate(values):
        mine = jnp.where(line == i, value, mine)
    sum_a[0] = mine
    sums_a = [
        remote(sum_a.at[0], sum_a.at[s], red_sem.at[2, 0, s], red_sem.at[2, 1, s], p)
        for s, p in group_a
    ]

    for c in range(3):
        for x in range(6):
            for k in range(3):
                t = k * 3 + c
                din[(c * 6 + x) * 8 : (c * 6 + x) * 8 + 8, k * 128 : k * 128 + 128] = pg[
                    t * 56 + x * 8 : t * 56 + x * 8 + 8, :
                ]
    whole = din[...]
    hi = whole.astype(BF16)
    rest = whole - hi.astype(F32)
    mid = rest.astype(BF16)
    lo = (rest - mid.astype(F32)).astype(BF16)
    perm = perm_ref[...]

    def back(x):
        return lax.dot_general(x, perm, (((1,), (1,)), ((), ())), preferred_element_type=F32)

    din[...] = back(hi) + (back(mid) + back(lo))
    for c in range(3):
        for x in range(6):
            grad_ref[c, x] = din[(c * 6 + x) * 8 : (c * 6 + x) * 8 + 6, :]
    leaving.append(pltpu.make_async_copy(grad_ref, grad_any, local_sem.at[7]))
    leaving[1].start()

    def weigh(ratio):
        two = ratio * ratio
        return jnp.where(
            line == 3,
            ratio,
            jnp.where(line == 4, two, jnp.where(line == 5, two * ratio, jnp.where(line == 6, two * two, 1.0))),
        )

    def pick(v, i):
        return jnp.sum(jnp.where(line == i, v, 0.0), axis=1, keepdims=True)

    def combine(ref, count):
        steps = [pick(ref[s], 2) for s in range(count)]
        least = functools.reduce(jnp.minimum, steps)
        out = jnp.zeros((1, 128), F32)
        for s in range(count):
            out = out + ref[s] * weigh(least / steps[s])
        return jnp.where(line == 2, least, out)

    for c in sums_a:
        c.wait_recv()
    sum_c[0] = combine(sum_a, count_a)
    sums_c = [
        remote(sum_c.at[0], sum_c.at[s], red_sem.at[5, 0, s], red_sem.at[5, 1, s], p)
        for s, p in group_c
    ]
    for c in sums_c:
        c.wait_recv()
    sum_b[0] = combine(sum_c, count_c)
    sums_b = [
        remote(sum_b.at[0], sum_b.at[s], red_sem.at[3, 0, s], red_sem.at[3, 1, s], p)
        for s, p in group_b
    ]
    for c in sums_b:
        c.wait_recv()
    final = combine(sum_b, count_b)
    square = pick(final, 1)
    step_length = TRIAL / jnp.sqrt(1.0 + square / entries)
    grown = final * weigh(step_length / pick(final, 2))
    elements = 512.0 * nx * ny * nz
    trial = jnp.sum(jnp.where((line == 0) | ((line >= 3) & (line < 7)), grown, 0.0))
    checks_ref[0] = jnp.sum(jnp.where(line == 0, final, 0.0)) * (1.0 / elements)
    checks_ref[1] = jnp.sum(jnp.where(line == 1, final, 0.0)) * (1.0 / entries)
    checks_ref[2] = trial * (1.0 / elements)

    for c in pending:
        c.wait_send()
    for c in leaving:
        c.wait()


def leave_kernel(a, b, c, to_a, to_b, to_c, sem):
    copies = [
        pltpu.make_async_copy(x, y, sem.at[i])
        for i, (x, y) in enumerate(((a, to_a), (b, to_b), (c, to_c)))
    ]
    for copy in copies:
        copy.start()
    for copy in copies:
        copy.wait()


def solution(mesh):
    nx, ny, nz = mesh.shape["gx"], mesh.shape["gy"], mesh.shape["gz"]
    _, wide = tables()
    hi, lo = halves(wide)
    wf = np.concatenate([hi, lo], axis=0)
    wb = np.concatenate([hi.T, lo.T], axis=0)
    perm = np.zeros((384, 384), np.float32)
    for k in range(3):
        perm[3 * np.arange(128) + k, k * 128 + np.arange(128)] = 1.0
    perm = perm.astype(jnp.bfloat16)
    count_a, count_b = ny * (nz // 2), nx
    most = max(count_a, count_b)
    anywhere = pl.BlockSpec(memory_space=pl.ANY)
    hbm = pl.BlockSpec(memory_space=pltpu.HBM)
    dma = pltpu.SemaphoreType.DMA
    call = pl.pallas_call(
        functools.partial(kernel, nx, ny, nz),
        name="tmop_step",
        out_shape=(
            jax.ShapeDtypeStruct((27, 4, 128), F32),
            jax.ShapeDtypeStruct((3, 6, 6, 384), F32),
            jax.ShapeDtypeStruct((3,), F32),
        ),
        in_specs=[hbm] * 6,
        out_specs=(hbm, hbm, pl.BlockSpec(memory_space=pltpu.SMEM)),
        scratch_shapes=[
            pltpu.VMEM((27, 4, 128), F32),
            pltpu.VMEM((3, 6, 6, 384), F32),
            pltpu.VMEM((3, 6, 6, 384), F32),
            pltpu.VMEM((27, 4, 128), F32),
            pltpu.VMEM((3, 4, 128), F32),
            pltpu.VMEM((64, 128), F32),
            pltpu.VMEM((1536, 224), BF16),
            pltpu.VMEM((448, 768), BF16),
            pltpu.VMEM((384, 384), BF16),
            pltpu.VMEM((2 * ROUNDS + 1, 3, 3, 3, 8, 128), F32),
            pltpu.VMEM((3, 8, 128), F32),
            pltpu.VMEM((2, 3, 8, 128), F32),
            pltpu.VMEM((2, 3, 8, 128), F32),
            pltpu.VMEM((ROUNDS, 4, 11, 8, 128), F32),
            pltpu.VMEM((ROUNDS, 4, 11, 8, 128), F32),
            pltpu.VMEM((ROUNDS, 4, 2, 8, 128), F32),
            pltpu.VMEM((ROUNDS, 4, 2, 8, 128), F32),
            pltpu.VMEM((11, 8, 128), F32),
            pltpu.VMEM((11, 8, 128), F32),
            pltpu.VMEM((80, 128), F32),
            pltpu.VMEM((80, 128), F32),
            pltpu.VMEM((32, 128), F32),
            pltpu.VMEM((32, 128), F32),
            pltpu.VMEM((144, 384), F32),
            pltpu.VMEM((504, 128), F32),
            pltpu.VMEM((504, 128), F32),
            pltpu.VMEM((224, 768), F32),
            pltpu.VMEM((768, 768), F32),
            pltpu.VMEM((512, 128), F32),
            pltpu.VMEM((256, 128), F32),
            pltpu.VMEM((256, 128), F32),
            pltpu.VMEM((768, 768), BF16),
            pltpu.VMEM((768, 768), BF16),
            pltpu.VMEM((560, 128), F32),
            pltpu.VMEM((2, 10, 8, 128), F32),
            pltpu.VMEM((2, 10, 8, 128), F32),
            pltpu.VMEM((2, 72, 128), F32),
            pltpu.VMEM((2, 72, 128), F32),
            pltpu.VMEM((4, 16, 128), F32),
            pltpu.VMEM((4, 16, 128), F32),
            pltpu.VMEM((224, 384), F32),
            pltpu.VMEM((768, 384), F32),
            pltpu.VMEM((count_a, 1, 128), F32),
            pltpu.VMEM((count_b, 1, 128), F32),
            pltpu.VMEM((count_a, 1, 128), F32),
            pltpu.VMEM((count_b, 1, 128), F32),
            pltpu.VMEM((2, 1, 128), F32),
            pltpu.VMEM((2, 1, 128), F32),
            pltpu.VMEM((3, 3, 3, 8, 128), F32),
            dma((8,)),
            dma((8,)),
            dma((ROUNDS, 2, 4)),
            dma((ROUNDS, 2, 4)),
            dma((2, 3)),
            dma((2, 8)),
            dma((6, 2, most)),
        ],
        compiler_params=pltpu.CompilerParams(
            collective_id=0, has_side_effects=True, vmem_limit_bytes=67_043_328
        ),
    )

    leave = pl.pallas_call(
        leave_kernel,
        name="leave",
        out_shape=(
            jax.ShapeDtypeStruct((27, 4, 128), F32),
            jax.ShapeDtypeStruct((3, 6, 6, 384), F32),
            jax.ShapeDtypeStruct((3,), F32),
        ),
        in_specs=[pl.BlockSpec(memory_space=pltpu.VMEM)] * 3,
        out_specs=(hbm,) * 3,
        scratch_shapes=[dma((3,))],
    )

    def on_device(displacement, size_field_modes, velocity):
        adv, grad, checks = call(
            displacement,
            size_field_modes.reshape(27, 4, 128),
            velocity.reshape(3, 4, 128),
            jnp.asarray(wf),
            jnp.asarray(wb),
            jnp.asarray(perm),
        )
        adv, grad, checks = leave(adv, grad, checks)
        return adv.reshape(27, 2, 2, 128), grad, checks

    spec = P(None, "gx", "gy", "gz")
    return jax.shard_map(
        on_device, mesh=mesh, in_specs=(spec, spec, spec), out_specs=(spec, spec, P()), check_vma=False
    )
```
